32 devices in a mesh: rows: 8 (over z, y), cols: 4 (over x, core).
Axes of the slice: x: 2, y: 2, z: 4, core: 2. Of those that a mesh axis runs over, the one named last changes fastest.
Arguments:
- blocks: bfloat16 [32, 4, 3, 128, 128], P('rows', 'cols'), may hold values from -1.1953125 to 1.1953125
- block_cols: int32 [32, 4, 3], P('rows', 'cols'), may hold values from 0 to 31, as said below
Outputs:
- square_blocks: bfloat16 [32, 4, 36, 128, 128], P('rows', 'cols')
- square_cols: int32 [32, 4, 36], P('rows', 'cols')
- square_start: int32 [32, 4], P('rows', 'cols')
The draws below stay inside these ranges and needn't reach their ends.
Inputs may be any that keep to these rules, and one draw needn't show every extreme that they name: Block-row i lies in panel p = i // 4; every block_cols[i, g, s] is a block-column congruent to g modulo 4 among block-rows 4 * (p - 4) to 4 * (p + 4) - 1, taken modulo 32; the three entries of one group differ; the block-columns i - 1, i and i + 1 (modulo 32) are always among a row's entries.
All inputs are finite; a program needn't handle non-finite values.
Results may differ from the reference program's by a relative error of at most 0.001.
Values may be sent and summed in bfloat16 or wider, within the bound.
No kernel may reach another device: no remote copies, remote signals or barrier semaphores. Data moves between devices by JAX's collectives and lax.ppermute only.
A program may use at most 64 MiB of HBM per device.

```python
import jax
import jax.numpy as jnp
from jax import lax

BS = 128
PB = 4
KG = 3
HP = 4
GROUPS = 4
NB = 32
K = 12


def draw_block_cols(key, part):
    row_ids = jnp.arange(NB, dtype=jnp.int32)
    panel = row_ids // PB
    window_base = (panel - HP) * PB % NB
    choices_count = 2 * HP * PB // GROUPS
    group_ids = jnp.arange(GROUPS, dtype=jnp.int32)
    residue = (group_ids[None, :] - window_base[:, None]) % GROUPS
    delta = (group_ids[None, :] - row_ids[:, None] + 1) % GROUPS
    has_band = delta <= 2
    band_col = (row_ids[:, None] - 1 + delta) % NB
    band_place = (band_col - window_base[:, None]) % NB // GROUPS
    key_pick = jax.random.fold_in(key, 11)
    key_jump = jax.random.fold_in(key, 23)
    key_extra = jax.random.fold_in(key, 37)
    picked = jax.random.randint(key_pick, (NB, GROUPS), 0, choices_count, dtype=jnp.int32)
    jumped = jax.random.randint(key_jump, (NB, GROUPS), 1, choices_count, dtype=jnp.int32)
    extra = jax.random.randint(key_extra, (NB, GROUPS), 1, choices_count - 1, dtype=jnp.int32)
    other_jump = 1 + (jumped - 1 + extra) % (choices_count - 1)
    first_place = jnp.where(has_band, band_place, picked)
    second_place = (first_place + jumped) % choices_count
    third_place = (first_place + other_jump) % choices_count
    first_col = (window_base[:, None] + first_place * GROUPS + residue) % NB
    second_col = (window_base[:, None] + second_place * GROUPS + residue) % NB
    third_col = (window_base[:, None] + third_place * GROUPS + residue) % NB
    return jnp.stack([first_col, second_col, third_col], axis=-1).astype(jnp.int32)


def steps_of(stream_key, shape, shards, low, high):
    level = 1.0
    for axis_at, shards_of in shards:
        draws = jax.random.uniform(jax.random.fold_in(jax.random.fold_in(stream_key, 6), axis_at), (shards_of,), jnp.float32, low / len(shards), high / len(shards))
        level = level * jnp.repeat(jnp.exp(draws), shape[axis_at] // shards_of).reshape((-1,) + (1,) * (len(shape) - 1 - axis_at))
    return level


def centred(rng, shape, deviation, bound, shards=(), kind=jnp.bfloat16):
    result = deviation * jax.random.normal(rng, shape, jnp.float32)
    if shards:
        result = result * steps_of(rng, shape, shards, -0.22, 0.18)
    return jnp.clip(result, -bound, bound).astype(kind)


def setup_inputs(seed: int = 0) -> dict:
    key_of = jax.random.split(jax.random.key(seed), 3)
    blocks = centred(key_of[0], (NB, GROUPS, KG, BS, BS), 0.2, 1.1953125, ((0, 8), (1, 4)))
    block_cols = draw_block_cols(jax.random.fold_in(key_of[2], 71), 0)
    return dict(blocks=blocks, block_cols=block_cols)


def unique_slots(candidates):
    width = candidates.shape[-1]
    ordered = jnp.sort(candidates, axis=-1)
    firsts = jnp.concatenate([jnp.ones(ordered.shape[:-1] + (1,), dtype=bool), ordered[..., 1:] != ordered[..., :-1]], axis=-1)
    marks = firsts.astype(jnp.int32)
    totals = jnp.sum(marks, axis=-1).astype(jnp.int32)
    ranking = jnp.sum(marks[..., None, :] * (ordered[..., None, :] < candidates[..., :, None]).astype(jnp.int32), axis=-1)
    places = jnp.cumsum(marks, axis=-1) - 1
    slot_ids = jnp.arange(width, dtype=jnp.int32)
    chosen = (places[..., None, :] == slot_ids[:, None]) & firsts[..., None, :]
    columns = jnp.sum(jnp.where(chosen, ordered[..., None, :], 0), axis=-1).astype(jnp.int32)
    columns = jnp.where(slot_ids < totals[..., None], columns, -1).astype(jnp.int32)
    onehot = (ranking[..., None, :] == slot_ids[:, None]).astype(jnp.float32)
    return columns, onehot, totals


def reference(blocks, block_cols):
    def one_row(row_index):
        named = block_cols[row_index].reshape(K).astype(jnp.int32)
        left = blocks[row_index].reshape(K, BS, BS).astype(jnp.float32)
        right_vals = blocks[named].astype(jnp.float32)
        right_cols = block_cols[named]
        products = jnp.einsum("tab,tgsbc->gtsac", left, right_vals, precision=lax.Precision.HIGHEST)
        candidates = jnp.transpose(right_cols, (1, 0, 2)).reshape(GROUPS, K * KG)
        columns, onehot, totals = unique_slots(candidates)
        merged = jnp.einsum("goq,gqac->goac", onehot, products.reshape(GROUPS, K * KG, BS, BS), precision=lax.Precision.HIGHEST)
        return merged.astype(jnp.bfloat16), columns, totals

    square_blocks, square_cols, counts = lax.map(one_row, jnp.arange(NB, dtype=jnp.int32))
    square_start = (jnp.cumsum(counts, axis=0) - counts).astype(jnp.int32)
    return square_blocks, square_cols, square_start
```

```python
import functools

import jax
import jax.numpy as jnp
from jax import lax
from jax.experimental import pallas as pl
from jax.experimental.pallas import tpu as pltpu
from jax.sharding import PartitionSpec as P


HP = 4
IDX = 16


VMEM = pl.BlockSpec(memory_space=pltpu.VMEM)
SMEM = pl.BlockSpec(memory_space=pltpu.SMEM)


def mask16(row, lane, value):
    seen = jnp.broadcast_to(row[:, lane : lane + 1], (16, 128))
    return jnp.where(seen == value, 1.0, 0.0).astype(jnp.bfloat16)


def stretch(tile, rows):
    return jnp.concatenate([tile] * (rows // 16), axis=0)


def accumulate(dims, pieces, base_ref, lrel_ref, left, lp_ref, d_ref, emit):
    groups, per_group, bs, bins, cycle = dims
    depth = groups * bs
    lrow = lrel_ref[0:1, :]
    for n, (number, parts) in enumerate(pieces):
        for m in range(groups):
            for j in range(groups):
                total = None
                for t in range(per_group):
                    at = ((m ^ j) * per_group + t) * bs
                    hit = mask16(lrow, (j * groups + m) * per_group + t, float(number))
                    term = left[j][at : at + bs, :] * stretch(hit, bs)
                    total = term if total is None else total + term
                lp_ref[m * bs : (m + 1) * bs, n * depth + j * bs : n * depth + (j + 1) * bs] = total
    rows_of = []
    for number, parts in pieces:
        for ref, held, at in parts:
            if at is not None:
                row = ref[at : at + 16, :].astype(jnp.float32)[0:1, :]
        if base_ref is not None:
            row = row - base_ref[0].astype(jnp.float32)
            row = jnp.where(row < 0, row + float(cycle), row)
        rows_of.append(row)
    for first in range(0, bins, 2):
        chunk = range(first, min(first + 2, bins))
        for n, (number, parts) in enumerate(pieces):
            for ref, held, at in parts:
                for place, j in enumerate(held):
                    for b in chunk:
                        total = None
                        for s in range(per_group):
                            start = (place * per_group + s) * bs
                            hit = mask16(rows_of[n], j * per_group + s, float(b))
                            term = ref[start : start + bs, :] * stretch(hit, bs)
                            total = term if total is None else total + term
                        d_ref[
                            n * depth + j * bs : n * depth + (j + 1) * bs, b * bs : (b + 1) * bs
                        ] = total
        lo, hi = first * bs, (first + len(chunk)) * bs
        emit(lo, hi, jnp.dot(lp_ref[...], d_ref[:, lo:hi], preferred_element_type=jnp.float32))


def unpack_refs(refs, layout, with_base):
    refs = list(refs)
    base_ref = refs.pop(0) if with_base else None
    lrel_ref = refs.pop(0)
    left = [refs.pop(0) for _ in range(4)]
    pieces = []
    for number, parts in layout:
        pieces.append((number, [(refs.pop(0), held, at) for held, at in parts]))
    return base_ref, lrel_ref, left, pieces, refs


def step_kernel(dims, layout, with_base, with_acc, *refs):
    base_ref, lrel_ref, left, pieces, rest = unpack_refs(refs, layout, with_base)
    acc_ref = rest.pop(0) if with_acc else None
    out_ref, lp_ref, d_ref = rest

    def emit(lo, hi, value):
        out_ref[:, lo:hi] = value if acc_ref is None else acc_ref[:, lo:hi] + value

    accumulate(dims, pieces, base_ref, lrel_ref, left, lp_ref, d_ref, emit)


def last_kernel(dims, layout, with_base, *refs):
    base_ref, lrel_ref, left, pieces, rest = unpack_refs(refs, layout, with_base)
    acc_ref, slot_ref, col_ref, _, out_ref, lp_ref, d_ref, stage_ref, sems = rest
    groups, _, bs, bins, _ = dims
    me = col_ref[0]
    copies = []

    def emit(lo, hi, value):
        value = (acc_ref[:, lo:hi] + value).astype(jnp.bfloat16)
        for b in range(lo // bs, hi // bs):
            for m in range(groups):
                k = m * bins + b
                at = b * bs - lo
                stage_ref[k] = value[m * bs : (m + 1) * bs, at : at + bs]
                row = m ^ me
                copy = pltpu.make_async_copy(
                    stage_ref.at[k], out_ref.at[row, slot_ref[row * bins + b]], sems.at[k]
                )
                copy.start()
                copies.append(copy)

    accumulate(dims, pieces, base_ref, lrel_ref, left, lp_ref, d_ref, emit)
    for copy in copies:
        copy.wait()


def call_step(dims, base, lrel, left, panels, acc):
    groups, _, bs, bins, _ = dims
    layout = [(number, [(held, at) for _, held, at in parts]) for number, parts in panels]
    arrays = [array for _, parts in panels for array, _, _ in parts]
    args, specs = [], []
    if base is not None:
        args, specs = [base], [SMEM]
    args += [lrel, *left, *arrays]
    specs += [VMEM] * (1 + len(left) + len(arrays))
    aliases = {}
    if acc is not None:
        aliases = {len(args): 0}
        args.append(acc)
        specs.append(VMEM)
    depth = groups * bs * len(panels)
    rows = groups * bs
    flops = 2 * rows * depth * bins * bs
    return pl.pallas_call(
        functools.partial(step_kernel, dims, layout, base is not None, acc is not None),
        out_shape=jax.ShapeDtypeStruct((rows, bins * bs), jnp.float32),
        in_specs=specs,
        out_specs=VMEM,
        scratch_shapes=[
            pltpu.VMEM((rows, depth), jnp.bfloat16),
            pltpu.VMEM((depth, bins * bs), jnp.bfloat16),
        ],
        input_output_aliases=aliases,
        cost_estimate=pl.CostEstimate(flops=flops, bytes_accessed=6_000_000, transcendentals=0),
    )(*args)


def call_last(dims, base, lrel, left, panels, acc, slots, col, empty):
    groups, _, bs, bins, _ = dims
    layout = [(number, [(held, at) for _, held, at in parts]) for number, parts in panels]
    arrays = [array for _, parts in panels for array, _, _ in parts]
    args, specs = [], []
    if base is not None:
        args, specs = [base], [SMEM]
    args += [lrel, *left, *arrays, acc, slots, col, empty]
    specs += [VMEM] * (2 + len(left) + len(arrays)) + [SMEM, SMEM, pl.BlockSpec(memory_space=pl.ANY)]
    depth = groups * bs * len(panels)
    rows = groups * bs
    flops = 2 * rows * depth * bins * bs
    return pl.pallas_call(
        functools.partial(last_kernel, dims, layout, base is not None),
        out_shape=jax.ShapeDtypeStruct(empty.shape, empty.dtype),
        in_specs=specs,
        out_specs=pl.BlockSpec(memory_space=pl.ANY),
        scratch_shapes=[
            pltpu.VMEM((rows, depth), jnp.bfloat16),
            pltpu.VMEM((depth, bins * bs), jnp.bfloat16),
            pltpu.VMEM((groups * bins, bs, bs), jnp.bfloat16),
            pltpu.SemaphoreType.DMA((groups * bins,)),
        ],
        input_output_aliases={len(args) - 1: 0},
        cost_estimate=pl.CostEstimate(flops=flops, bytes_accessed=6_000_000, transcendentals=0),
        name="last",
    )(*args)


def xor_move(value, axis, bit):
    route = [(i, i ^ bit) for i in range(lax.axis_size(axis))]
    return lax.ppermute(value, axis, route)


def shifted(value, axis, distance):
    size = lax.axis_size(axis)
    route = [((i - distance) % size, i) for i in range(size)]
    return lax.ppermute(value, axis, route)


def one_of(values, wanted):
    return jnp.any(values[..., None] == wanted, axis=-2)


def on_device(blocks, block_cols):
    panel_rows, _, per_group, bs, _ = blocks.shape
    groups = lax.axis_size("cols")
    cycle = lax.axis_size("rows")
    slots_out = groups * per_group * per_group
    if groups != 4 or panel_rows != groups or cycle > 256 or cycle < 2 * HP:
        raise ValueError("unsupported sizes")
    bins = min(cycle, 4 * HP - 1)
    whole = cycle == 2 * HP and bins == cycle
    dims = (groups, per_group, bs, bins, cycle)
    p = lax.axis_index("rows").astype(jnp.int32)
    c = lax.axis_index("cols").astype(jnp.int32)
    lanes = jnp.arange(groups, dtype=jnp.int32)
    body_rows = groups * per_group * bs

    mine = block_cols[:, 0] // groups
    order = lanes ^ c
    numbers = mine[order].astype(jnp.bfloat16).reshape(1, groups * per_group)
    numbers = jnp.pad(numbers, ((0, IDX - 1), (0, bs - groups * per_group)))
    body = jnp.concatenate(
        [lax.dynamic_index_in_dim(blocks[:, 0], c ^ j, 0, keepdims=False) for j in range(groups)], axis=0
    ).reshape(body_rows, bs)
    own = jnp.concatenate([body, numbers], axis=0)
    every = list(range(groups))

    def full(array):
        return [(array, every, body_rows)]

    if whole:
        x1 = xor_move(own, "rows", 2)
        x2 = xor_move(own, "rows", 4)
        y0 = xor_move(own, "rows", 1)
    else:
        window = [own if k == 0 else shifted(own, "rows", -k) for k in range(-HP, HP)]
    left1 = xor_move(own, "cols", 1)
    left2 = xor_move(own, "cols", 2)
    left3 = xor_move(left2, "cols", 1)
    left = [own, left1, left2, left3]

    def numbers_of(array, count=groups * per_group):
        return array[body_rows, :count].astype(jnp.int32)

    held = jnp.stack(
        [numbers_of(left[j]).reshape(groups, per_group)[jnp.array([m ^ j for m in every])] for j in every],
        axis=1,
    )
    if whole:
        lrel = held ^ p
        base = None
        zero = jnp.int32(0)
    else:
        lrel = (held - (p - HP)) % cycle
        zero = (p - 2 * HP) % cycle if bins < cycle else jnp.int32(0)
        base = zero.reshape(1)
    lrel_row = jnp.transpose(lrel, (1, 0, 2)).reshape(1, groups * groups * per_group)
    lrel_row = jnp.pad(lrel_row.astype(jnp.float32), ((0, 7), (0, 128 - lrel_row.shape[1])))
    bin_ids = jnp.arange(bins, dtype=jnp.int32)
    bin_abs = (zero + bin_ids) % cycle

    if whole:
        yx1 = xor_move(x1, "rows", 1)
        x12 = xor_move(x2, "rows", 2)
        yx2 = xor_move(x2, "rows", 1)
        half = groups // 2
        cut = half * per_group * bs
        tail_a = xor_move(x12[:cut], "rows", 1)
        tail_b = xor_move(yx2[cut:], "rows", 2)
        known = held.reshape(1, -1)
        for bit in (4, 2, 1):
            known = jnp.concatenate([known, xor_move(known, "rows", bit)], axis=0)
        places = jnp.array([0, 4, 2, 6, 1, 5, 3, 7], dtype=jnp.int32)
        panel_of = places ^ p
        known = known.reshape(cycle, groups, groups, per_group)
        uses = one_of(known, panel_of)
        has = one_of(known[:, :, 0, :], bin_ids)
        hits = jnp.any(
            uses.transpose(0, 1, 3, 2)[..., None] & has[None, None], axis=(2, 3)
        )
        totals = jnp.sum(hits.astype(jnp.int32), axis=-1)
        earlier = jnp.sum(jnp.where((panel_of < p)[:, None], totals, 0))
        mine_hits = hits[0]
        acc = call_step(dims, base, lrel_row, left, [(0, full(own)), (2, full(x1)), (1, full(y0))], None)
        acc = call_step(dims, base, lrel_row, left, [(3, full(yx1)), (4, full(x2))], acc)
        acc = call_step(dims, base, lrel_row, left, [(5, full(yx2)), (6, full(x12))], acc)
        final = [(7, [(tail_a, every[:half], None), (tail_b, every[half:], cut)])]
    else:
        has = jnp.stack(
            [one_of((numbers_of(w).reshape(groups, per_group) - zero) % cycle, bin_ids) for w in window]
        )
        uses = one_of(lrel, jnp.arange(2 * HP, dtype=jnp.int32))
        mine_hits = jnp.any(uses.transpose(0, 2, 1)[..., None] & has[None], axis=(1, 2))
        panel_total = jnp.sum(mine_hits.astype(jnp.int32))
        all_totals = lax.all_gather(panel_total.reshape(1), "rows", axis=0, tiled=True)
        earlier = jnp.sum(jnp.where(jnp.arange(cycle, dtype=jnp.int32) < p, all_totals, 0))
        acc = None
        for at in (0, 2, 4):
            acc = call_step(dims, base, lrel_row, left, [(e, full(window[e])) for e in (at, at + 1)], acc)
        final = [(e, full(window[e])) for e in (6, 7)]

    pick = (lanes[:, None] ^ c) == lanes[None, :]
    present = jnp.any(pick[:, :, None] & mine_hits[None], axis=1)
    lower = bin_abs[:, None] < bin_abs[None, :]
    counts = jnp.sum(present.astype(jnp.int32), axis=-1)
    rank_in = jnp.sum((present[:, :, None] & lower[None]).astype(jnp.int32), axis=1)
    rank_out = jnp.sum((~present[:, :, None] & lower[None]).astype(jnp.int32), axis=1)
    slots = jnp.where(present, rank_in, counts[:, None] + rank_out)
    at_slot = present[:, None, :] & (slots[:, None, :] == jnp.arange(slots_out, dtype=jnp.int32)[:, None])
    columns = jnp.sum(jnp.where(at_slot, bin_abs * groups + c + 1, 0), axis=-1) - 1
    before = lanes[:, None] > lanes[None, :]
    starts = earlier + jnp.sum(jnp.where(before, counts[None, :], 0), axis=1)

    empty = jnp.zeros((panel_rows, slots_out, bs, bs), jnp.bfloat16)
    out = call_last(dims, base, lrel_row, left, final, acc, slots.reshape(-1), c.reshape(1), empty)
    return out[:, None], columns.astype(jnp.int32)[:, None], starts.astype(jnp.int32)[:, None]


def solution(mesh):
    in_specs = (P("rows", "cols", None, None, None), P("rows", "cols", None))
    out_specs = (P("rows", "cols", None, None, None), P("rows", "cols", None), P("rows", "cols"))

    return jax.shard_map(on_device, mesh=mesh, in_specs=in_specs, out_specs=out_specs, check_vma=False)
```

```python
import functools

import jax
import jax.numpy as jnp
from jax import lax
from jax.experimental import pallas as pl
from jax.experimental.pallas import tpu as pltpu
from jax.sharding import PartitionSpec as P


HP = 4
IDX = 16


VMEM = pl.BlockSpec(memory_space=pltpu.VMEM)
SMEM = pl.BlockSpec(memory_space=pltpu.SMEM)
ANY = pl.BlockSpec(memory_space=pl.ANY)
GRANT = 20 * 1024 * 1024


class Dims:
    def __init__(self, groups, per_group, bs, bins, cycle):
        self.groups, self.per_group, self.bs = groups, per_group, bs
        self.bins, self.cycle = bins, cycle
        self.half = groups // 2 * per_group * bs
        self.rows = groups * bs
        self.slots = groups * per_group * per_group
        self.whole = cycle == 2 * HP and bins == cycle

    def at(self, j, s):
        return (j * self.per_group + s) * self.bs + (IDX if j >= self.groups // 2 else 0)


def ring_place(panel, cycle):
    return jnp.where(panel % 2 == 0, panel // 2, cycle - 1 - panel // 2)


def panel_number(dims, distance):
    me = lax.axis_index("rows").astype(jnp.int32)
    if not dims.whole:
        return (me + distance + dims.cycle) % dims.cycle
    place = (ring_place(me, dims.cycle) + distance + dims.cycle) % dims.cycle
    return jnp.where(place < dims.cycle // 2, 2 * place, 2 * (dims.cycle - 1 - place) + 1)


def first_bin(dims):
    me = lax.axis_index("rows").astype(jnp.int32)
    return (me - 2 * HP + 2 * dims.cycle) % dims.cycle


def stretch(tile, rows):
    return jnp.concatenate([tile] * (rows // 16), axis=0)


def prep_kernel(dims, blocks_ref, cols_ref, full_ref, a_ref, b_ref):
    me = lax.axis_index("cols").astype(jnp.int32)
    bs = dims.bs
    lane = lax.broadcasted_iota(jnp.int32, (IDX, 128), 1)
    row = jnp.zeros((IDX, 128), jnp.int32)
    for j in range(dims.groups):
        for s in range(dims.per_group):
            value = blocks_ref[me ^ j, 0, s]
            at = dims.at(j, s)
            full_ref[at : at + bs, :] = value
            if at < dims.half:
                a_ref[at : at + bs, :] = value
            else:
                at -= dims.half + IDX
                b_ref[at : at + bs, :] = value
            row = jnp.where(lane == j * dims.per_group + s, cols_ref[me ^ j, 0, s] // dims.groups, row)
    numbers = row.astype(jnp.float32).astype(jnp.bfloat16)
    full_ref[dims.half : dims.half + IDX, :] = numbers
    a_ref[dims.half : dims.half + IDX, :] = numbers


def accumulate(dims, pieces, left, lp_ref, d_ref, emit):
    groups, per_group, bs, bins = dims.groups, dims.per_group, dims.bs, dims.bins
    depth = dims.rows
    lrows = [ref[dims.half : dims.half + 16, :].astype(jnp.float32)[0:1, :] for ref in left]
    for n, (distance, _, _) in enumerate(pieces):
        number = panel_number(dims, distance).astype(jnp.float32)
        for j in range(groups):
            hits = jnp.where(lrows[j] == number, 1.0, 0.0)
            for m in range(groups):
                total = None
                for t in range(per_group):
                    at = dims.at(m ^ j, t)
                    lane = (m ^ j) * per_group + t
                    hit = jnp.broadcast_to(hits[:, lane : lane + 1], (16, 128)).astype(jnp.bfloat16)
                    term = left[j][at : at + bs, :] * stretch(hit, bs)
                    total = term if total is None else total + term
                lp_ref[m * bs : (m + 1) * bs, n * depth + j * bs : n * depth + (j + 1) * bs] = total
    rows_of = []
    for _, ref, _ in pieces:
        row = ref[dims.half : dims.half + 16, :].astype(jnp.float32)[0:1, :]
        if dims.bins < dims.cycle:
            row = row - first_bin(dims).astype(jnp.float32)
            row = jnp.where(row < 0, row + float(dims.cycle), row)
        rows_of.append(row)
    for first in range(0, bins, 2):
        chunk = range(first, min(first + 2, bins))
        for n, (_, a_ref, b_ref) in enumerate(pieces):
            for b in chunk:
                hits = jnp.where(rows_of[n] == float(b), 1.0, 0.0)
                for j in range(groups):
                    total = None
                    for s in range(per_group):
                        ref, start = a_ref, dims.at(j, s)
                        if b_ref is not None and j >= groups // 2:
                            ref, start = b_ref, start - dims.half - IDX
                        lane = j * per_group + s
                        hit = jnp.broadcast_to(hits[:, lane : lane + 1], (16, 128)).astype(jnp.bfloat16)
                        term = ref[start : start + bs, :] * stretch(hit, bs)
                        total = term if total is None else total + term
                    d_ref[
                        n * depth + j * bs : n * depth + (j + 1) * bs, b * bs : (b + 1) * bs
                    ] = total
        lo, hi = first * bs, (first + len(chunk)) * bs
        emit(lo, hi, jnp.dot(lp_ref[...], d_ref[:, lo:hi], preferred_element_type=jnp.float32))


def take(refs, count):
    return [refs.pop(0) for _ in range(count)]


def take_pieces(refs, layout):
    pieces = []
    for distance, two in layout:
        pieces.append((distance, refs.pop(0), refs.pop(0) if two else None))
    return pieces


def step_kernel(dims, layout, with_acc, with_zero, *refs):
    refs = list(refs)
    left = take(refs, dims.groups)
    pieces = take_pieces(refs, layout)
    acc_ref = refs.pop(0) if with_acc else None
    out_ref = refs.pop(0)
    zero_ref = refs.pop(0) if with_zero else None
    lp_ref, d_ref = take(refs, 2)
    copies = []
    if with_zero:
        blank_ref, sems = refs
        blank_ref[...] = jnp.zeros_like(blank_ref)
        for i in range(zero_ref.shape[0]):
            copy = pltpu.make_async_copy(
                blank_ref, zero_ref.at[i, dims.bins : dims.slots], sems.at[i]
            )
            copy.start()
            copies.append(copy)

    def emit(lo, hi, value):
        out_ref[:, lo:hi] = value if acc_ref is None else acc_ref[:, lo:hi] + value

    accumulate(dims, pieces, left, lp_ref, d_ref, emit)
    for copy in copies:
        copy.wait()


def last_kernel(dims, layout, *refs):
    refs = list(refs)
    left = take(refs, dims.groups)
    pieces = take_pieces(refs, layout)
    acc_ref, slot_ref, _, out_ref, lp_ref, d_ref, stage_ref, sems = refs
    groups, bs, bins = dims.groups, dims.bs, dims.bins
    me = lax.axis_index("cols").astype(jnp.int32)
    copies = []

    def emit(lo, hi, value):
        value = (acc_ref[:, lo:hi] + value).astype(jnp.bfloat16)
        for b in range(lo // bs, hi // bs):
            for m in range(groups):
                k = m * bins + b
                at = b * bs - lo
                stage_ref[k] = value[m * bs : (m + 1) * bs, at : at + bs]
                copy = pltpu.make_async_copy(
                    stage_ref.at[k], out_ref.at[m ^ me, slot_ref[k]], sems.at[k]
                )
                copy.start()
                copies.append(copy)

    accumulate(dims, pieces, left, lp_ref, d_ref, emit)
    for copy in copies:
        copy.wait()


def index_kernel(dims, known_ref, slot_ref, cols_ref, start_ref, mask_ref, count_ref):
    groups, per_group, bins, cycle = dims.groups, dims.per_group, dims.bins, dims.cycle
    p = lax.axis_index("rows").astype(jnp.int32)
    c = lax.axis_index("cols").astype(jnp.int32)
    places = hyper_places(cycle)
    for n in range(cycle):
        for r in range(groups):
            bits = jnp.int32(0)
            for s in range(per_group):
                bits = bits | (jnp.int32(1) << known_ref[n * groups, r * per_group + s])
            mask_ref[(p ^ places[n]) * groups + r] = bits
    earlier = jnp.int32(0)
    for n in range(cycle):
        total = jnp.int32(0)
        for m in range(groups):
            bits = jnp.int32(0)
            for j in range(groups):
                for t in range(per_group):
                    k = known_ref[n * groups + j, (m ^ j) * per_group + t]
                    bits = bits | mask_ref[k * groups + j]
            count = jnp.int32(0)
            for b in range(bins):
                count = count + ((bits >> b) & 1)
            total = total + count
            if n == 0:
                count_ref[m ^ c] = count
                used = jnp.int32(0)
                for b in range(bins):
                    one = (bits >> b) & 1
                    slot = jnp.where(one == 1, used, count + b - used)
                    slot_ref[m * bins + b] = slot
                    cols_ref[m ^ c, 0, slot] = jnp.where(one == 1, b * groups + c, -1)
                    used = used + one
        if n > 0:
            earlier = earlier + jnp.where((p ^ places[n]) < p, total, 0)
    for i in range(groups):
        start_ref[i, 0] = earlier
        earlier = earlier + count_ref[i]
        for o in range(bins, dims.slots):
            cols_ref[i, 0, o] = -1


def hyper_bits(cycle):
    bits, bit = [], cycle // 2
    while bit:
        bits.append(bit)
        bit //= 2
    return bits


def hyper_places(cycle):
    places = [0]
    for bit in hyper_bits(cycle):
        places = places + [v ^ bit for v in places]
    return places


def flat(panels):
    layout = [(distance, second is not None) for distance, _, second in panels]
    arrays = [x for _, first, second in panels for x in (first, second) if x is not None]
    return layout, arrays


def scratch_of(dims, panels):
    depth = dims.rows * len(panels)
    return [
        pltpu.VMEM((dims.rows, depth), jnp.bfloat16),
        pltpu.VMEM((depth, dims.bins * dims.bs), jnp.bfloat16),
    ]


def cost_of(dims, panels):
    flops = 2 * dims.rows * dims.rows * len(panels) * dims.bins * dims.bs
    return pl.CostEstimate(flops=flops, bytes_accessed=4_000_000, transcendentals=0)


def call_step(dims, left, panels, acc, zero=False):
    layout, arrays = flat(panels)
    args = [*left, *arrays]
    aliases = {}
    if acc is not None:
        aliases = {len(args): 0}
        args.append(acc)
    shapes = [jax.ShapeDtypeStruct((dims.rows, dims.bins * dims.bs), jnp.float32)]
    specs = [VMEM]
    scratch = scratch_of(dims, panels)
    if zero:
        shapes.append(
            jax.ShapeDtypeStruct((dims.groups, dims.slots, dims.bs, dims.bs), jnp.bfloat16)
        )
        specs.append(ANY)
        scratch += [
            pltpu.VMEM((dims.slots - dims.bins, dims.bs, dims.bs), jnp.bfloat16),
            pltpu.SemaphoreType.DMA((dims.groups,)),
        ]
    return pl.pallas_call(
        functools.partial(step_kernel, dims, layout, acc is not None, zero),
        out_shape=shapes,
        in_specs=[VMEM] * len(args),
        out_specs=specs,
        scratch_shapes=scratch,
        input_output_aliases=aliases,
        compiler_params=pltpu.CompilerParams(vmem_limit_bytes=GRANT),
        cost_estimate=cost_of(dims, panels),
    )(*args)


def call_last(dims, left, panels, acc, slots, empty):
    layout, arrays = flat(panels)
    args = [*left, *arrays, acc, slots, empty]
    return pl.pallas_call(
        functools.partial(last_kernel, dims, layout),
        out_shape=jax.ShapeDtypeStruct(empty.shape, empty.dtype),
        in_specs=[VMEM] * (len(args) - 2) + [SMEM, ANY],
        out_specs=ANY,
        scratch_shapes=scratch_of(dims, panels)
        + [
            pltpu.VMEM((dims.groups * dims.bins, dims.bs, dims.bs), jnp.bfloat16),
            pltpu.SemaphoreType.DMA((dims.groups * dims.bins,)),
        ],
        input_output_aliases={len(args) - 1: 0},
        compiler_params=pltpu.CompilerParams(vmem_limit_bytes=GRANT),
        cost_estimate=cost_of(dims, panels),
    )(*args)


def xor_move(value, axis, bit):
    return lax.ppermute(value, axis, [(i, i ^ bit) for i in range(lax.axis_size(axis))])


def shifted(value, axis, distance):
    size = lax.axis_size(axis)
    return lax.ppermute(value, axis, [((i - distance) % size, i) for i in range(size)])


def ring_moves(cycle):
    ring = [2 * k for k in range(cycle // 2)] + [2 * k + 1 for k in reversed(range(cycle // 2))]
    up = [(ring[k], ring[(k + 1) % cycle]) for k in range(cycle)]
    return up, [(b, a) for a, b in up]


def one_of(values, wanted):
    return jnp.any(values[..., None] == wanted, axis=-2)


def window_index(dims, left, window):
    groups, per_group, bins, cycle = dims.groups, dims.per_group, dims.bins, dims.cycle
    p = lax.axis_index("rows").astype(jnp.int32)
    c = lax.axis_index("cols").astype(jnp.int32)
    lanes = jnp.arange(groups, dtype=jnp.int32)

    def numbers_of(array):
        numbers = array[dims.half, : groups * per_group].astype(jnp.int32)
        return numbers.reshape(groups, per_group)

    held = jnp.stack(
        [numbers_of(left[j])[jnp.array([m ^ j for m in range(groups)])] for j in range(groups)], axis=1
    )
    lrel = (held - (p - HP)) % cycle
    zero = (p - 2 * HP) % cycle if bins < cycle else jnp.int32(0)
    bin_ids = jnp.arange(bins, dtype=jnp.int32)
    bin_abs = (zero + bin_ids) % cycle
    has = jnp.stack([one_of((numbers_of(w) - zero) % cycle, bin_ids) for w in window])
    uses = one_of(lrel, jnp.arange(2 * HP, dtype=jnp.int32))
    hits = jnp.any(uses.transpose(0, 2, 1)[..., None] & has[None], axis=(1, 2))
    counts = jnp.sum(hits.astype(jnp.int32), axis=-1)
    all_totals = lax.all_gather(jnp.sum(counts).reshape(1), "rows", axis=0, tiled=True)
    earlier = jnp.sum(jnp.where(jnp.arange(cycle, dtype=jnp.int32) < p, all_totals, 0))
    lower = bin_abs[:, None] < bin_abs[None, :]
    rank_in = jnp.sum((hits[:, :, None] & lower[None]).astype(jnp.int32), axis=1)
    rank_out = jnp.sum((~hits[:, :, None] & lower[None]).astype(jnp.int32), axis=1)
    slots = jnp.where(hits, rank_in, counts[:, None] + rank_out)
    at_slot = hits[:, None, :] & (slots[:, None, :] == jnp.arange(dims.slots, dtype=jnp.int32)[:, None])
    columns = jnp.sum(jnp.where(at_slot, bin_abs * groups + c + 1, 0), axis=-1) - 1
    pick = (lanes[:, None] ^ c) == lanes[None, :]
    columns = jnp.sum(jnp.where(pick[:, :, None], columns[None], 0), axis=1)
    before = (lanes[None, :] ^ c) < lanes[:, None]
    starts = earlier + jnp.sum(jnp.where(before, counts[None, :], 0), axis=1)
    return slots.reshape(-1), columns[:, None].astype(jnp.int32), starts[:, None].astype(jnp.int32)


def on_device(blocks, block_cols):
    panel_rows, _, per_group, bs, _ = blocks.shape
    groups = lax.axis_size("cols")
    cycle = lax.axis_size("rows")
    if groups != 4 or panel_rows != groups or cycle > 256 or cycle < 2 * HP:
        raise ValueError("unsupported sizes")
    dims = Dims(groups, per_group, bs, min(cycle, 4 * HP - 1), cycle)

    def payload(rows):
        return jax.ShapeDtypeStruct((rows, bs), jnp.bfloat16)

    own, own_a, own_b = pl.pallas_call(
        functools.partial(prep_kernel, dims),
        out_shape=[payload(2 * dims.half + IDX), payload(dims.half + IDX), payload(dims.half)],
        in_specs=[VMEM, SMEM],
        out_specs=[VMEM] * 3,
        compiler_params=pltpu.CompilerParams(vmem_limit_bytes=GRANT),
        name="prep",
    )(blocks, block_cols)

    if dims.whole:
        up, down = ring_moves(cycle)
        pa, pb, qa, qb = [own_a], [own_b], [own_a], [own_b]
        for k in range(1, HP + 1):
            pa.append(lax.ppermute(pa[-1], "rows", up))
            qb.append(lax.ppermute(qb[-1], "rows", down))
            if k < HP:
                pb.append(lax.ppermute(pb[-1], "rows", up))
                qa.append(lax.ppermute(qa[-1], "rows", down))
    else:
        window = [own if k == 0 else shifted(own, "rows", -k) for k in range(-HP, HP)]
    left1 = xor_move(own, "cols", 1)
    left2 = xor_move(own, "cols", 2)
    left3 = xor_move(left2, "cols", 1)
    left = [own, left1, left2, left3]

    if dims.whole:
        known = jnp.concatenate([x[dims.half : dims.half + 1] for x in left], axis=0)
        for bit in hyper_bits(cycle):
            known = jnp.concatenate([known, xor_move(known, "rows", bit)], axis=0)
        known = known[:, : groups * per_group].astype(jnp.int32)
        slots, columns, starts = pl.pallas_call(
            functools.partial(index_kernel, dims),
            out_shape=[
                jax.ShapeDtypeStruct((groups * dims.bins,), jnp.int32),
                jax.ShapeDtypeStruct((groups, 1, dims.slots), jnp.int32),
                jax.ShapeDtypeStruct((groups, 1), jnp.int32),
            ],
            in_specs=[SMEM],
            out_specs=[SMEM] * 3,
            scratch_shapes=[
                pltpu.SMEM((cycle * groups,), jnp.int32),
                pltpu.SMEM((groups,), jnp.int32),
            ],
            compiler_params=pltpu.CompilerParams(vmem_limit_bytes=GRANT),
            name="index",
        )(known)
        acc, empty = call_step(dims, left, [(0, own, None)], None, zero=True)
        for k in range(1, HP):
            panels = [(-k, pa[k], pb[k]), (k, qa[k], qb[k])]
            acc = call_step(dims, left, panels, acc)[0]
        final = [(HP, pa[HP], qb[HP])]
    else:
        slots, columns, starts = window_index(dims, left, window)
        acc, empty = call_step(dims, left, [(0, own, None)], None, zero=True)
        pairs = [(k, window[k + HP], None) for k in range(-HP, HP) if k]
        for k in range(0, len(pairs) - 1, 2):
            acc = call_step(dims, left, pairs[k : k + 2], acc)[0]
        final = pairs[-1:]
    out = call_last(dims, left, final, acc, slots, empty)
    return out[:, None], columns, starts


def solution(mesh):
    in_specs = (P("rows", "cols", None, None, None), P("rows", "cols", None))
    out_specs = (P("rows", "cols", None, None, None), P("rows", "cols", None), P("rows", "cols"))

    return jax.shard_map(on_device, mesh=mesh, in_specs=in_specs, out_specs=out_specs, check_vma=False)
```

```python
import functools

import jax
import jax.numpy as jnp
from jax import lax
from jax.experimental import pallas as pl
from jax.experimental.pallas import tpu as pltpu
from jax.sharding import PartitionSpec as P


HP = 4
IDX = 16


VMEM = pl.BlockSpec(memory_space=pltpu.VMEM)
SMEM = pl.BlockSpec(memory_space=pltpu.SMEM)
ANY = pl.BlockSpec(memory_space=pl.ANY)
HBM = pl.BlockSpec(memory_space=pltpu.HBM)
GRANT = 12 * 1024 * 1024


class Dims:
    def __init__(self, groups, per_group, bs, bins, cycle):
        self.groups, self.per_group, self.bs = groups, per_group, bs
        self.bins, self.cycle = bins, cycle
        self.half = groups // 2 * per_group * bs
        self.rows = groups * bs
        self.slots = groups * per_group * per_group
        self.whole = cycle == 2 * HP and bins == cycle

    def at(self, j, s):
        return (j * self.per_group + s) * self.bs + (IDX if j >= self.groups // 2 else 0)


def ring_place(panel, cycle):
    return jnp.where(panel % 2 == 0, panel // 2, cycle - 1 - panel // 2)


def panel_number(dims, distance):
    me = lax.axis_index("rows").astype(jnp.int32)
    if not dims.whole:
        return (me + distance + dims.cycle) % dims.cycle
    place = (ring_place(me, dims.cycle) + distance + dims.cycle) % dims.cycle
    return jnp.where(place < dims.cycle // 2, 2 * place, 2 * (dims.cycle - 1 - place) + 1)


def first_bin(dims):
    me = lax.axis_index("rows").astype(jnp.int32)
    return (me - 2 * HP + 2 * dims.cycle) % dims.cycle


def stretch(tile, rows):
    return jnp.concatenate([tile] * (rows // 16), axis=0)


def prep_kernel(dims, blocks_ref, cols_ref, full_ref, a_ref, b_ref, sems):
    me = lax.axis_index("cols").astype(jnp.int32)
    span = dims.per_group * dims.bs
    copies = []
    for j in range(dims.groups):
        at = dims.at(j, 0)
        ref, start = (a_ref, at) if at < dims.half else (b_ref, at - dims.half - IDX)
        for k, (out_ref, first) in enumerate(((ref, start), (full_ref, at))):
            copy = pltpu.make_async_copy(
                blocks_ref.at[pl.ds((me ^ j) * span, span)], out_ref.at[first : first + span], sems.at[j, k]
            )
            copy.start()
            copies.append(copy)
    lane = lax.broadcasted_iota(jnp.int32, (IDX, 128), 1)
    row = jnp.zeros((IDX, 128), jnp.int32)
    for j in range(dims.groups):
        for s in range(dims.per_group):
            row = jnp.where(lane == j * dims.per_group + s, cols_ref[s, 0, me ^ j] // dims.groups, row)
    numbers = row.astype(jnp.float32).astype(jnp.bfloat16)
    full_ref[dims.half : dims.half + IDX, :] = numbers
    a_ref[dims.half : dims.half + IDX, :] = numbers
    for copy in copies:
        copy.wait()


def accumulate(dims, pieces, left, lp_ref, d_ref, emit):
    groups, per_group, bs, bins = dims.groups, dims.per_group, dims.bs, dims.bins
    depth = dims.rows
    lrows = [ref[dims.half : dims.half + 16, :].astype(jnp.float32)[0:1, :] for ref in left]
    for n, (distance, _, _) in enumerate(pieces):
        number = panel_number(dims, distance).astype(jnp.float32)
        for j in range(groups):
            hits = jnp.where(lrows[j] == number, 1.0, 0.0)
            for m in range(groups):
                total = None
                for t in range(per_group):
                    at = dims.at(m ^ j, t)
                    lane = (m ^ j) * per_group + t
                    hit = jnp.broadcast_to(hits[:, lane : lane + 1], (16, 128)).astype(jnp.bfloat16)
                    term = left[j][at : at + bs, :] * stretch(hit, bs)
                    total = term if total is None else total + term
                lp_ref[m * bs : (m + 1) * bs, n * depth + j * bs : n * depth + (j + 1) * bs] = total
    rows_of = []
    for _, ref, _ in pieces:
        row = ref[dims.half : dims.half + 16, :].astype(jnp.float32)[0:1, :]
        if dims.bins < dims.cycle:
            row = row - first_bin(dims).astype(jnp.float32)
            row = jnp.where(row < 0, row + float(dims.cycle), row)
        rows_of.append(row)
    for first in range(0, bins, 2):
        chunk = range(first, min(first + 2, bins))
        for n, (_, a_ref, b_ref) in enumerate(pieces):
            for b in chunk:
                hits = jnp.where(rows_of[n] == float(b), 1.0, 0.0)
                for j in range(groups):
                    total = None
                    for s in range(per_group):
                        ref, start = a_ref, dims.at(j, s)
                        if b_ref is not None and j >= groups // 2:
                            ref, start = b_ref, start - dims.half - IDX
                        lane = j * per_group + s
                        hit = jnp.broadcast_to(hits[:, lane : lane + 1], (16, 128)).astype(jnp.bfloat16)
                        term = ref[start : start + bs, :] * stretch(hit, bs)
                        total = term if total is None else total + term
                    d_ref[
                        n * depth + j * bs : n * depth + (j + 1) * bs, b * bs : (b + 1) * bs
                    ] = total
        lo, hi = first * bs, (first + len(chunk)) * bs
        emit(lo, hi, jnp.dot(lp_ref[...], d_ref[:, lo:hi], preferred_element_type=jnp.float32))


def take(refs, count):
    return [refs.pop(0) for _ in range(count)]


def take_pieces(refs, layout):
    pieces = []
    for distance, two in layout:
        pieces.append((distance, refs.pop(0), refs.pop(0) if two else None))
    return pieces


def step_kernel(dims, layout, with_acc, with_zero, *refs):
    refs = list(refs)
    left = take(refs, dims.groups)
    pieces = take_pieces(refs, layout)
    acc_ref = refs.pop(0) if with_acc else None
    out_ref = refs.pop(0)
    zero_ref = refs.pop(0) if with_zero else None
    lp_ref, d_ref = take(refs, 2)
    copies = []
    if with_zero:
        blank_ref, sems = refs
        blank_ref[...] = jnp.zeros_like(blank_ref)
        for i in range(zero_ref.shape[0]):
            copy = pltpu.make_async_copy(
                blank_ref, zero_ref.at[i, dims.bins : dims.slots], sems.at[i]
            )
            copy.start()
            copies.append(copy)

    def emit(lo, hi, value):
        out_ref[:, lo:hi] = value if acc_ref is None else acc_ref[:, lo:hi] + value

    accumulate(dims, pieces, left, lp_ref, d_ref, emit)
    for copy in copies:
        copy.wait()


def last_kernel(dims, layout, *refs):
    refs = list(refs)
    left = take(refs, dims.groups)
    pieces = take_pieces(refs, layout)
    acc_ref, slot_ref, _, out_ref, lp_ref, d_ref, stage_ref, sems = refs
    groups, bs, bins = dims.groups, dims.bs, dims.bins
    me = lax.axis_index("cols").astype(jnp.int32)
    copies = []

    def emit(lo, hi, value):
        value = (acc_ref[:, lo:hi] + value).astype(jnp.bfloat16)
        for b in range(lo // bs, hi // bs):
            for m in range(groups):
                k = m * bins + b
                at = b * bs - lo
                stage_ref[k] = value[m * bs : (m + 1) * bs, at : at + bs]
                copy = pltpu.make_async_copy(
                    stage_ref.at[k], out_ref.at[m ^ me, slot_ref[k]], sems.at[k]
                )
                copy.start()
                copies.append(copy)

    accumulate(dims, pieces, left, lp_ref, d_ref, emit)
    for copy in copies:
        copy.wait()


def index_kernel(dims, known_ref, slot_ref, cols_ref, start_ref, mask_ref, count_ref):
    groups, per_group, bins, cycle = dims.groups, dims.per_group, dims.bins, dims.cycle
    p = lax.axis_index("rows").astype(jnp.int32)
    c = lax.axis_index("cols").astype(jnp.int32)
    number = [panel_number(dims, n if n <= HP else n - cycle) for n in range(cycle)]
    for n in range(cycle):
        for r in range(groups):
            bits = jnp.int32(0)
            for s in range(per_group):
                bits = bits | (jnp.int32(1) << known_ref[n * groups, r * per_group + s])
            mask_ref[number[n] * groups + r] = bits
    earlier = jnp.int32(0)
    for n in range(cycle):
        total = jnp.int32(0)
        for m in range(groups):
            bits = jnp.int32(0)
            for j in range(groups):
                for t in range(per_group):
                    k = known_ref[n * groups + j, (m ^ j) * per_group + t]
                    bits = bits | mask_ref[k * groups + j]
            count = jnp.int32(0)
            for b in range(bins):
                count = count + ((bits >> b) & 1)
            total = total + count
            if n == 0:
                count_ref[m ^ c] = count
                used = jnp.int32(0)
                for b in range(bins):
                    one = (bits >> b) & 1
                    slot = jnp.where(one == 1, used, count + b - used)
                    slot_ref[m * bins + b] = slot
                    cols_ref[m ^ c, 0, slot] = jnp.where(one == 1, b * groups + c, -1)
                    used = used + one
        if n > 0:
            earlier = earlier + jnp.where(number[n] < p, total, 0)
    for i in range(groups):
        start_ref[0, i] = earlier
        earlier = earlier + count_ref[i]
        for o in range(bins, dims.slots):
            cols_ref[i, 0, o] = -1


def flat(panels):
    layout = [(distance, second is not None) for distance, _, second in panels]
    arrays = [x for _, first, second in panels for x in (first, second) if x is not None]
    return layout, arrays


def scratch_of(dims, panels):
    depth = dims.rows * len(panels)
    return [
        pltpu.VMEM((dims.rows, depth), jnp.bfloat16),
        pltpu.VMEM((depth, dims.bins * dims.bs), jnp.bfloat16),
    ]


def cost_of(dims, panels):
    flops = 2 * dims.rows * dims.rows * len(panels) * dims.bins * dims.bs
    return pl.CostEstimate(flops=flops, bytes_accessed=4_000_000, transcendentals=0)


def call_step(dims, left, panels, acc, zero=False):
    layout, arrays = flat(panels)
    args = [*left, *arrays]
    aliases = {}
    if acc is not None:
        aliases = {len(args): 0}
        args.append(acc)
    shapes = [jax.ShapeDtypeStruct((dims.rows, dims.bins * dims.bs), jnp.float32)]
    specs = [VMEM]
    scratch = scratch_of(dims, panels)
    if zero:
        shapes.append(
            jax.ShapeDtypeStruct((dims.groups, dims.slots, dims.bs, dims.bs), jnp.bfloat16)
        )
        specs.append(ANY)
        scratch += [
            pltpu.VMEM((dims.slots - dims.bins, dims.bs, dims.bs), jnp.bfloat16),
            pltpu.SemaphoreType.DMA((dims.groups,)),
        ]
    return pl.pallas_call(
        functools.partial(step_kernel, dims, layout, acc is not None, zero),
        out_shape=shapes,
        in_specs=[VMEM] * len(args),
        out_specs=specs,
        scratch_shapes=scratch,
        input_output_aliases=aliases,
        compiler_params=pltpu.CompilerParams(vmem_limit_bytes=GRANT),
        cost_estimate=cost_of(dims, panels),
    )(*args)


def call_last(dims, left, panels, acc, slots, empty):
    layout, arrays = flat(panels)
    args = [*left, *arrays, acc, slots, empty]
    return pl.pallas_call(
        functools.partial(last_kernel, dims, layout),
        out_shape=jax.ShapeDtypeStruct(empty.shape, empty.dtype),
        in_specs=[VMEM] * (len(args) - 2) + [SMEM, ANY],
        out_specs=ANY,
        scratch_shapes=scratch_of(dims, panels)
        + [
            pltpu.VMEM((dims.groups * dims.bins, dims.bs, dims.bs), jnp.bfloat16),
            pltpu.SemaphoreType.DMA((dims.groups * dims.bins,)),
        ],
        input_output_aliases={len(args) - 1: 0},
        compiler_params=pltpu.CompilerParams(vmem_limit_bytes=GRANT),
        cost_estimate=cost_of(dims, panels),
    )(*args)


def xor_move(value, axis, bit):
    return lax.ppermute(value, axis, [(i, i ^ bit) for i in range(lax.axis_size(axis))])


def shifted(value, axis, distance):
    size = lax.axis_size(axis)
    return lax.ppermute(value, axis, [((i - distance) % size, i) for i in range(size)])


def ring_moves(cycle):
    ring = [2 * k for k in range(cycle // 2)] + [2 * k + 1 for k in reversed(range(cycle // 2))]
    up = [(ring[k], ring[(k + 1) % cycle]) for k in range(cycle)]
    return up, [(b, a) for a, b in up]


def one_of(values, wanted):
    return jnp.any(values[..., None] == wanted, axis=-2)


def window_index(dims, left, window):
    groups, per_group, bins, cycle = dims.groups, dims.per_group, dims.bins, dims.cycle
    p = lax.axis_index("rows").astype(jnp.int32)
    c = lax.axis_index("cols").astype(jnp.int32)
    lanes = jnp.arange(groups, dtype=jnp.int32)

    def numbers_of(array):
        numbers = array[dims.half, : groups * per_group].astype(jnp.int32)
        return numbers.reshape(groups, per_group)

    held = jnp.stack(
        [numbers_of(left[j])[jnp.array([m ^ j for m in range(groups)])] for j in range(groups)], axis=1
    )
    lrel = (held - (p - HP)) % cycle
    zero = (p - 2 * HP) % cycle if bins < cycle else jnp.int32(0)
    bin_ids = jnp.arange(bins, dtype=jnp.int32)
    bin_abs = (zero + bin_ids) % cycle
    has = jnp.stack([one_of((numbers_of(w) - zero) % cycle, bin_ids) for w in window])
    uses = one_of(lrel, jnp.arange(2 * HP, dtype=jnp.int32))
    hits = jnp.any(uses.transpose(0, 2, 1)[..., None] & has[None], axis=(1, 2))
    counts = jnp.sum(hits.astype(jnp.int32), axis=-1)
    all_totals = lax.all_gather(jnp.sum(counts).reshape(1), "rows", axis=0, tiled=True)
    earlier = jnp.sum(jnp.where(jnp.arange(cycle, dtype=jnp.int32) < p, all_totals, 0))
    lower = bin_abs[:, None] < bin_abs[None, :]
    rank_in = jnp.sum((hits[:, :, None] & lower[None]).astype(jnp.int32), axis=1)
    rank_out = jnp.sum((~hits[:, :, None] & lower[None]).astype(jnp.int32), axis=1)
    slots = jnp.where(hits, rank_in, counts[:, None] + rank_out)
    at_slot = hits[:, None, :] & (slots[:, None, :] == jnp.arange(dims.slots, dtype=jnp.int32)[:, None])
    columns = jnp.sum(jnp.where(at_slot, bin_abs * groups + c + 1, 0), axis=-1) - 1
    pick = (lanes[:, None] ^ c) == lanes[None, :]
    columns = jnp.sum(jnp.where(pick[:, :, None], columns[None], 0), axis=1)
    before = (lanes[None, :] ^ c) < lanes[:, None]
    starts = earlier + jnp.sum(jnp.where(before, counts[None, :], 0), axis=1)
    return slots.reshape(-1), columns[:, None].astype(jnp.int32), starts[:, None].astype(jnp.int32)


def on_device(blocks, block_cols):
    panel_rows, _, per_group, bs, _ = blocks.shape
    groups = lax.axis_size("cols")
    cycle = lax.axis_size("rows")
    if groups != 4 or panel_rows != groups or cycle > 256 or cycle < 2 * HP:
        raise ValueError("unsupported sizes")
    dims = Dims(groups, per_group, bs, min(cycle, 4 * HP - 1), cycle)

    def payload(rows):
        return jax.ShapeDtypeStruct((rows, bs), jnp.bfloat16)

    own, own_a, own_b = pl.pallas_call(
        functools.partial(prep_kernel, dims),
        out_shape=[payload(2 * dims.half + IDX), payload(dims.half + IDX), payload(dims.half)],
        in_specs=[HBM, SMEM],
        out_specs=[VMEM] * 3,
        scratch_shapes=[
            pltpu.SemaphoreType.DMA((groups, 2)),
        ],
        compiler_params=pltpu.CompilerParams(vmem_limit_bytes=GRANT),
        name="prep",
    )(blocks.reshape(-1, bs), jnp.transpose(block_cols, (2, 1, 0)))

    if dims.whole:
        up, down = ring_moves(cycle)
        pa, pb, qa, qb = [own_a], [own_b], [own_a], [own_b]
        for k in range(1, HP + 1):
            pa.append(lax.ppermute(pa[-1], "rows", up))
            qb.append(lax.ppermute(qb[-1], "rows", down))
            if k < HP:
                pb.append(lax.ppermute(pb[-1], "rows", up))
                qa.append(lax.ppermute(qa[-1], "rows", down))
    else:
        window = [own if k == 0 else shifted(own, "rows", -k) for k in range(-HP, HP)]
    left1 = xor_move(own, "cols", 1)
    left2 = xor_move(own, "cols", 2)
    left3 = xor_move(left2, "cols", 1)
    left = [own, left1, left2, left3]

    if dims.whole:
        heard = {0: jnp.concatenate([x[dims.half : dims.half + 1] for x in left], axis=0)}
        for k in range(1, HP + 1):
            heard[-k] = lax.ppermute(heard[1 - k], "rows", up)
            if k < HP:
                heard[k] = lax.ppermute(heard[k - 1], "rows", down)
        order = [0, 1, 2, 3, -4, -3, -2, -1]
        known = jnp.concatenate([heard[k] for k in order], axis=0)
        known = known[:, : groups * per_group].astype(jnp.int32)
        slots, columns, starts = pl.pallas_call(
            functools.partial(index_kernel, dims),
            out_shape=[
                jax.ShapeDtypeStruct((groups * dims.bins,), jnp.int32),
                jax.ShapeDtypeStruct((groups, 1, dims.slots), jnp.int32),
                jax.ShapeDtypeStruct((1, groups), jnp.int32),
            ],
            in_specs=[SMEM],
            out_specs=[SMEM] * 3,
            scratch_shapes=[
                pltpu.SMEM((cycle * groups,), jnp.int32),
                pltpu.SMEM((groups,), jnp.int32),
            ],
            compiler_params=pltpu.CompilerParams(vmem_limit_bytes=GRANT),
            name="index",
        )(known)
        starts = starts.reshape(groups, 1)
        pairs = [[(-k, pa[k], pb[k]), (k, qa[k], qb[k])] for k in range(1, HP)]
        acc, empty = call_step(dims, left, [(0, own, None)] + pairs[0], None, zero=True)
        for k in range(2, HP):
            acc = call_step(dims, left, pairs[k - 1], acc)[0]
        final = [(HP, pa[HP], qb[HP])]
    else:
        slots, columns, starts = window_index(dims, left, window)
        acc, empty = call_step(dims, left, [(0, own, None)], None, zero=True)
        pairs = [(k, window[k + HP], None) for k in range(-HP, HP) if k]
        for k in range(0, len(pairs) - 1, 2):
            acc = call_step(dims, left, pairs[k : k + 2], acc)[0]
        final = pairs[-1:]
    out = call_last(dims, left, final, acc, slots, empty)
    return out[:, None], columns, starts


def solution(mesh):
    in_specs = (P("rows", "cols", None, None, None), P("rows", "cols", None))
    out_specs = (P("rows", "cols", None, None, None), P("rows", "cols", None), P("rows", "cols"))

    return jax.shard_map(on_device, mesh=mesh, in_specs=in_specs, out_specs=out_specs, check_vma=False)
```

```python
import functools

import jax
import jax.numpy as jnp
from jax import lax
from jax.experimental import pallas as pl
from jax.experimental.pallas import tpu as pltpu
from jax.sharding import PartitionSpec as P


HP = 4
IDX = 16


VMEM = pl.BlockSpec(memory_space=pltpu.VMEM)
SMEM = pl.BlockSpec(memory_space=pltpu.SMEM)
ANY = pl.BlockSpec(memory_space=pl.ANY)
HBM = pl.BlockSpec(memory_space=pltpu.HBM)
GRANT = 12 * 1024 * 1024


class Dims:
    def __init__(self, groups, per_group, bs, bins, cycle):
        self.groups, self.per_group, self.bs = groups, per_group, bs
        self.bins, self.cycle = bins, cycle
        self.half = groups // 2 * per_group * bs
        self.rows = groups * bs
        self.slots = groups * per_group * per_group
        self.whole = cycle == 2 * HP and bins == cycle

    def at(self, j, s):
        return (j * self.per_group + s) * self.bs + (IDX if j >= self.groups // 2 else 0)


def ring_place(panel, cycle):
    return jnp.where(panel % 2 == 0, panel // 2, cycle - 1 - panel // 2)


def panel_number(dims, distance):
    me = lax.axis_index("rows").astype(jnp.int32)
    if not dims.whole:
        return (me + distance + dims.cycle) % dims.cycle
    place = (ring_place(me, dims.cycle) + distance + dims.cycle) % dims.cycle
    return jnp.where(place < dims.cycle // 2, 2 * place, 2 * (dims.cycle - 1 - place) + 1)


def first_bin(dims):
    me = lax.axis_index("rows").astype(jnp.int32)
    return (me - 2 * HP + 2 * dims.cycle) % dims.cycle


def stretch(tile, rows):
    return jnp.concatenate([tile] * (rows // 16), axis=0)


def prep_kernel(dims, *refs):
    refs = list(refs)
    cols = take(refs, dims.groups)
    blocks_ref, full_ref, a_ref, b_ref, tile_ref, sems = refs
    me = lax.axis_index("cols").astype(jnp.int32)
    span = dims.per_group * dims.bs
    copies = []
    for j in range(dims.groups):
        at = dims.at(j, 0)
        ref, start = (a_ref, at) if at < dims.half else (b_ref, at - dims.half - IDX)
        for k, (out_ref, first) in enumerate(((ref, start), (full_ref, at))):
            copy = pltpu.make_async_copy(
                blocks_ref.at[pl.ds((me ^ j) * span, span)], out_ref.at[first : first + span], sems.at[j, k]
            )
            copy.start()
            copies.append(copy)
    line = lax.broadcasted_iota(jnp.int32, (IDX, 128), 0)
    lane = lax.broadcasted_iota(jnp.int32, (IDX, 128), 1)
    tile = jnp.zeros((IDX, 128), jnp.int32)
    for j in range(dims.groups):
        row = jnp.zeros((IDX, 128), jnp.int32)
        for r in range(dims.groups):
            for s in range(dims.per_group):
                number = cols[j][s, 0, me ^ j ^ r] // dims.groups
                row = jnp.where(lane == r * dims.per_group + s, number, row)
        tile = jnp.where(line == j, row, tile)
    numbers = tile.astype(jnp.float32).astype(jnp.bfloat16)
    tile_ref[...] = numbers
    for ref in (a_ref, b_ref):
        ref[dims.half : dims.half + IDX, :] = numbers
    for at in (dims.half, 2 * dims.half + IDX):
        full_ref[at : at + IDX, :] = numbers
    for copy in copies:
        copy.wait()


def accumulate(dims, pieces, left, lp_ref, d_ref, emit):
    groups, per_group, bs, bins = dims.groups, dims.per_group, dims.bs, dims.bins
    depth = dims.rows
    lrows = [ref[dims.half : dims.half + 16, :].astype(jnp.float32)[0:1, :] for ref in left]
    for n, (distance, _, _) in enumerate(pieces):
        number = panel_number(dims, distance).astype(jnp.float32)
        for j in range(groups):
            hits = jnp.where(lrows[j] == number, 1.0, 0.0)
            for m in range(groups):
                total = None
                for t in range(per_group):
                    at = dims.at(m ^ j, t)
                    lane = (m ^ j) * per_group + t
                    hit = jnp.broadcast_to(hits[:, lane : lane + 1], (16, 128)).astype(jnp.bfloat16)
                    term = left[j][at : at + bs, :] * stretch(hit, bs)
                    total = term if total is None else total + term
                lp_ref[m * bs : (m + 1) * bs, n * depth + j * bs : n * depth + (j + 1) * bs] = total
    rows_of = []
    for _, ref, _ in pieces:
        row = ref[dims.half : dims.half + 16, :].astype(jnp.float32)[0:1, :]
        if dims.bins < dims.cycle:
            row = row - first_bin(dims).astype(jnp.float32)
            row = jnp.where(row < 0, row + float(dims.cycle), row)
        rows_of.append(row)
    for first in range(0, bins, 2):
        chunk = range(first, min(first + 2, bins))
        for n, (_, a_ref, b_ref) in enumerate(pieces):
            for b in chunk:
                hits = jnp.where(rows_of[n] == float(b), 1.0, 0.0)
                for j in range(groups):
                    total = None
                    for s in range(per_group):
                        ref, start = a_ref, dims.at(j, s)
                        if b_ref is not None and j >= groups // 2:
                            ref, start = b_ref, start - dims.half - IDX
                        lane = j * per_group + s
                        hit = jnp.broadcast_to(hits[:, lane : lane + 1], (16, 128)).astype(jnp.bfloat16)
                        term = ref[start : start + bs, :] * stretch(hit, bs)
                        total = term if total is None else total + term
                    d_ref[
                        n * depth + j * bs : n * depth + (j + 1) * bs, b * bs : (b + 1) * bs
                    ] = total
        lo, hi = first * bs, (first + len(chunk)) * bs
        emit(lo, hi, jnp.dot(lp_ref[...], d_ref[:, lo:hi], preferred_element_type=jnp.float32))


def take(refs, count):
    return [refs.pop(0) for _ in range(count)]


def take_pieces(refs, layout):
    pieces = []
    for distance, two in layout:
        pieces.append((distance, refs.pop(0), refs.pop(0) if two else None))
    return pieces


def step_kernel(dims, layout, with_acc, with_zero, tiles, *refs):
    refs = list(refs)
    left = take(refs, dims.groups)
    pieces = take_pieces(refs, layout)
    tile_refs = take(refs, len(tiles))
    acc_ref = refs.pop(0) if with_acc else None
    out_ref = refs.pop(0)
    zero_ref = refs.pop(0) if with_zero else None
    index_refs = take(refs, 3) if tiles else None
    lp_ref, d_ref = take(refs, 2)
    copies = []
    if with_zero:
        blank_ref, sems = refs
        blank_ref[...] = jnp.zeros_like(blank_ref)
        for i in range(zero_ref.shape[0]):
            copy = pltpu.make_async_copy(
                blank_ref, zero_ref.at[i, dims.bins : dims.slots], sems.at[i]
            )
            copy.start()
            copies.append(copy)
    if tiles:
        wide_ref, known_ref, mask_ref, count_ref, sem = refs
        for k, (n, at) in enumerate(tiles):
            tile = tile_refs[k][at : at + IDX, :].astype(jnp.float32).astype(jnp.int32)
            wide_ref[n * 8 : (n + 1) * 8, :] = tile[:8]
        known = pltpu.make_async_copy(wide_ref, known_ref, sem)
        known.start()

    def emit(lo, hi, value):
        out_ref[:, lo:hi] = value if acc_ref is None else acc_ref[:, lo:hi] + value
        if tiles and lo == 0:
            known.wait()
            index_work(dims, known_ref, *index_refs, mask_ref, count_ref)

    accumulate(dims, pieces, left, lp_ref, d_ref, emit)
    for copy in copies:
        copy.wait()


def last_kernel(dims, layout, *refs):
    refs = list(refs)
    left = take(refs, dims.groups)
    pieces = take_pieces(refs, layout)
    acc_ref, slot_ref, _, out_ref, lp_ref, d_ref, stage_ref, sems = refs
    groups, bs, bins = dims.groups, dims.bs, dims.bins
    me = lax.axis_index("cols").astype(jnp.int32)
    copies = []

    def emit(lo, hi, value):
        value = (acc_ref[:, lo:hi] + value).astype(jnp.bfloat16)
        for b in range(lo // bs, hi // bs):
            for m in range(groups):
                k = m * bins + b
                at = b * bs - lo
                stage_ref[k] = value[m * bs : (m + 1) * bs, at : at + bs]
                copy = pltpu.make_async_copy(
                    stage_ref.at[k], out_ref.at[m ^ me, slot_ref[k]], sems.at[k]
                )
                copy.start()
                copies.append(copy)

    accumulate(dims, pieces, left, lp_ref, d_ref, emit)
    for copy in copies:
        copy.wait()


def index_work(dims, known_ref, slot_ref, cols_ref, start_ref, mask_ref, count_ref):
    groups, per_group, bins, cycle = dims.groups, dims.per_group, dims.bins, dims.cycle
    p = lax.axis_index("rows").astype(jnp.int32)
    c = lax.axis_index("cols").astype(jnp.int32)
    number = [panel_number(dims, n if n <= HP else n - cycle) for n in range(cycle)]
    for n in range(cycle):
        for r in range(groups):
            bits = jnp.int32(0)
            for s in range(per_group):
                bits = bits | (jnp.int32(1) << known_ref[n * 8, r * per_group + s])
            mask_ref[number[n] * groups + r] = bits
    earlier = jnp.int32(0)
    for n in range(cycle):
        total = jnp.int32(0)
        for m in range(groups):
            bits = jnp.int32(0)
            for j in range(groups):
                for t in range(per_group):
                    k = known_ref[n * 8 + j, (m ^ j) * per_group + t]
                    bits = bits | mask_ref[k * groups + j]
            count = jnp.int32(0)
            for b in range(bins):
                count = count + ((bits >> b) & 1)
            total = total + count
            if n == 0:
                count_ref[m ^ c] = count
                used = jnp.int32(0)
                for b in range(bins):
                    one = (bits >> b) & 1
                    slot = jnp.where(one == 1, used, count + b - used)
                    slot_ref[m * bins + b] = slot
                    cols_ref[m ^ c, 0, slot] = jnp.where(one == 1, b * groups + c, -1)
                    used = used + one
        if n > 0:
            earlier = earlier + jnp.where(number[n] < p, total, 0)
    for i in range(groups):
        start_ref[0, i] = earlier
        earlier = earlier + count_ref[i]
        for o in range(bins, dims.slots):
            cols_ref[i, 0, o] = -1


def flat(panels):
    layout = [(distance, second is not None) for distance, _, second in panels]
    arrays = [x for _, first, second in panels for x in (first, second) if x is not None]
    return layout, arrays


def scratch_of(dims, panels):
    depth = dims.rows * len(panels)
    return [
        pltpu.VMEM((dims.rows, depth), jnp.bfloat16),
        pltpu.VMEM((depth, dims.bins * dims.bs), jnp.bfloat16),
    ]


def cost_of(dims, panels):
    flops = 2 * dims.rows * dims.rows * len(panels) * dims.bins * dims.bs
    return pl.CostEstimate(flops=flops, bytes_accessed=4_000_000, transcendentals=0)


def call_step(dims, left, panels, acc, zero=False, tiles=()):
    layout, arrays = flat(panels)
    args = [*left, *arrays, *(array for _, array, _ in tiles)]
    aliases = {}
    if acc is not None:
        aliases = {len(args): 0}
        args.append(acc)
    shapes = [jax.ShapeDtypeStruct((dims.rows, dims.bins * dims.bs), jnp.float32)]
    specs = [VMEM]
    scratch = scratch_of(dims, panels)
    if zero:
        shapes.append(
            jax.ShapeDtypeStruct((dims.groups, dims.slots, dims.bs, dims.bs), jnp.bfloat16)
        )
        specs.append(ANY)
        scratch += [
            pltpu.VMEM((dims.slots - dims.bins, dims.bs, dims.bs), jnp.bfloat16),
            pltpu.SemaphoreType.DMA((dims.groups,)),
        ]
    if tiles:
        shapes += [
            jax.ShapeDtypeStruct((dims.groups * dims.bins,), jnp.int32),
            jax.ShapeDtypeStruct((dims.groups, 1, dims.slots), jnp.int32),
            jax.ShapeDtypeStruct((1, dims.groups), jnp.int32),
        ]
        specs += [SMEM] * 3
        scratch += [
            pltpu.VMEM((dims.cycle * 8, 128), jnp.int32),
            pltpu.SMEM((dims.cycle * 8, 128), jnp.int32),
            pltpu.SMEM((dims.cycle * dims.groups,), jnp.int32),
            pltpu.SMEM((dims.groups,), jnp.int32),
            pltpu.SemaphoreType.DMA,
        ]
    marks = tuple((n, at) for n, _, at in tiles)
    return pl.pallas_call(
        functools.partial(step_kernel, dims, layout, acc is not None, zero, marks),
        out_shape=shapes,
        in_specs=[VMEM] * len(args),
        out_specs=specs,
        scratch_shapes=scratch,
        input_output_aliases=aliases,
        compiler_params=pltpu.CompilerParams(vmem_limit_bytes=GRANT),
        cost_estimate=cost_of(dims, panels),
    )(*args)


def call_last(dims, left, panels, acc, slots, empty):
    layout, arrays = flat(panels)
    args = [*left, *arrays, acc, slots, empty]
    return pl.pallas_call(
        functools.partial(last_kernel, dims, layout),
        out_shape=jax.ShapeDtypeStruct(empty.shape, empty.dtype),
        in_specs=[VMEM] * (len(args) - 2) + [SMEM, ANY],
        out_specs=ANY,
        scratch_shapes=scratch_of(dims, panels)
        + [
            pltpu.VMEM((dims.groups * dims.bins, dims.bs, dims.bs), jnp.bfloat16),
            pltpu.SemaphoreType.DMA((dims.groups * dims.bins,)),
        ],
        input_output_aliases={len(args) - 1: 0},
        compiler_params=pltpu.CompilerParams(vmem_limit_bytes=GRANT),
        cost_estimate=cost_of(dims, panels),
    )(*args)


def xor_move(value, axis, bit):
    return lax.ppermute(value, axis, [(i, i ^ bit) for i in range(lax.axis_size(axis))])


def shifted(value, axis, distance):
    size = lax.axis_size(axis)
    return lax.ppermute(value, axis, [((i - distance) % size, i) for i in range(size)])


def ring_moves(cycle):
    ring = [2 * k for k in range(cycle // 2)] + [2 * k + 1 for k in reversed(range(cycle // 2))]
    up = [(ring[k], ring[(k + 1) % cycle]) for k in range(cycle)]
    return up, [(b, a) for a, b in up]


def one_of(values, wanted):
    return jnp.any(values[..., None] == wanted, axis=-2)


def window_index(dims, left, window):
    groups, per_group, bins, cycle = dims.groups, dims.per_group, dims.bins, dims.cycle
    p = lax.axis_index("rows").astype(jnp.int32)
    c = lax.axis_index("cols").astype(jnp.int32)
    lanes = jnp.arange(groups, dtype=jnp.int32)

    def numbers_of(array):
        numbers = array[dims.half, : groups * per_group].astype(jnp.int32)
        return numbers.reshape(groups, per_group)

    held = jnp.stack(
        [numbers_of(left[j])[jnp.array([m ^ j for m in range(groups)])] for j in range(groups)], axis=1
    )
    lrel = (held - (p - HP)) % cycle
    zero = (p - 2 * HP) % cycle if bins < cycle else jnp.int32(0)
    bin_ids = jnp.arange(bins, dtype=jnp.int32)
    bin_abs = (zero + bin_ids) % cycle
    has = jnp.stack([one_of((numbers_of(w) - zero) % cycle, bin_ids) for w in window])
    uses = one_of(lrel, jnp.arange(2 * HP, dtype=jnp.int32))
    hits = jnp.any(uses.transpose(0, 2, 1)[..., None] & has[None], axis=(1, 2))
    counts = jnp.sum(hits.astype(jnp.int32), axis=-1)
    all_totals = lax.all_gather(jnp.sum(counts).reshape(1), "rows", axis=0, tiled=True)
    earlier = jnp.sum(jnp.where(jnp.arange(cycle, dtype=jnp.int32) < p, all_totals, 0))
    lower = bin_abs[:, None] < bin_abs[None, :]
    rank_in = jnp.sum((hits[:, :, None] & lower[None]).astype(jnp.int32), axis=1)
    rank_out = jnp.sum((~hits[:, :, None] & lower[None]).astype(jnp.int32), axis=1)
    slots = jnp.where(hits, rank_in, counts[:, None] + rank_out)
    at_slot = hits[:, None, :] & (slots[:, None, :] == jnp.arange(dims.slots, dtype=jnp.int32)[:, None])
    columns = jnp.sum(jnp.where(at_slot, bin_abs * groups + c + 1, 0), axis=-1) - 1
    pick = (lanes[:, None] ^ c) == lanes[None, :]
    columns = jnp.sum(jnp.where(pick[:, :, None], columns[None], 0), axis=1)
    before = (lanes[None, :] ^ c) < lanes[:, None]
    starts = earlier + jnp.sum(jnp.where(before, counts[None, :], 0), axis=1)
    return slots.reshape(-1), columns[:, None].astype(jnp.int32), starts[:, None].astype(jnp.int32)


def on_device(blocks, block_cols):
    panel_rows, _, per_group, bs, _ = blocks.shape
    groups = lax.axis_size("cols")
    cycle = lax.axis_size("rows")
    if groups != 4 or panel_rows != groups or cycle > 256 or cycle < 2 * HP:
        raise ValueError("unsupported sizes")
    dims = Dims(groups, per_group, bs, min(cycle, 4 * HP - 1), cycle)

    def payload(rows):
        return jax.ShapeDtypeStruct((rows, bs), jnp.bfloat16)

    cols = [block_cols] + [xor_move(block_cols, "cols", j) for j in range(1, groups)]
    own, own_a, own_b, tile = pl.pallas_call(
        functools.partial(prep_kernel, dims),
        out_shape=[payload(2 * dims.half + 2 * IDX)] + [payload(dims.half + IDX)] * 2 + [payload(IDX)],
        in_specs=[SMEM] * groups + [ANY],
        out_specs=[VMEM] * 4,
        scratch_shapes=[pltpu.SemaphoreType.DMA((groups, 2))],
        compiler_params=pltpu.CompilerParams(vmem_limit_bytes=GRANT),
        name="prep",
    )(*(jnp.transpose(x, (2, 1, 0)) for x in cols), blocks.reshape(-1, bs))

    if dims.whole:
        up, down = ring_moves(cycle)
        pa, pb, qa, qb = [own_a], [own_b], [own_a], [own_b]
        for k in range(1, HP + 1):
            pa.append(lax.ppermute(pa[-1], "rows", up))
            qb.append(lax.ppermute(qb[-1], "rows", down))
            if k < HP:
                pb.append(lax.ppermute(pb[-1], "rows", up))
                qa.append(lax.ppermute(qa[-1], "rows", down))
    else:
        window = [own if k == 0 else shifted(own, "rows", -k) for k in range(-HP, HP)]
    left1 = xor_move(own, "cols", 1)
    left2 = xor_move(own, "cols", 2)
    left3 = xor_move(left2, "cols", 1)
    left = [own, left1, left2, left3]

    if dims.whole:
        far = lax.ppermute(tile, "rows", [(a, dict(up)[dict(up)[dict(up)[b]]]) for a, b in up])
        pairs = [[(-k, pa[k], pb[k]), (k, qa[k], qb[k])] for k in range(1, HP)]
        acc, empty = call_step(dims, left, [(0, own, None)] + pairs[0], None, zero=True)
        for k in range(2, HP - 1):
            acc = call_step(dims, left, pairs[k - 1], acc)[0]
        tiles = [(0, tile, 0), (HP, far, 0)]
        for k in range(1, HP):
            tiles += [(cycle - k, pa[k], dims.half), (k, qb[k], dims.half)]
        acc, slots, columns, starts = call_step(dims, left, pairs[-1], acc, tiles=tiles)
        starts = starts.reshape(groups, 1)
        final = [(HP, pa[HP], qb[HP])]
    else:
        slots, columns, starts = window_index(dims, left, window)
        acc, empty = call_step(dims, left, [(0, own, None)], None, zero=True)
        pairs = [(k, window[k + HP], None) for k in range(-HP, HP) if k]
        for k in range(0, len(pairs) - 1, 2):
            acc = call_step(dims, left, pairs[k : k + 2], acc)[0]
        final = pairs[-1:]
    out = call_last(dims, left, final, acc, slots, empty)
    return out[:, None], columns, starts


def solution(mesh):
    in_specs = (P("rows", "cols", None, None, None), P("rows", "cols", None))
    out_specs = (P("rows", "cols", None, None, None), P("rows", "cols", None), P("rows", "cols"))

    return jax.shard_map(on_device, mesh=mesh, in_specs=in_specs, out_specs=out_specs, check_vma=False)
```

```python
import functools

import jax
import jax.numpy as jnp
from jax import lax
from jax.experimental import pallas as pl
from jax.experimental.pallas import tpu as pltpu
from jax.sharding import PartitionSpec as P


HP = 4
IDX = 16


VMEM = pl.BlockSpec(memory_space=pltpu.VMEM)
SMEM = pl.BlockSpec(memory_space=pltpu.SMEM)
ANY = pl.BlockSpec(memory_space=pl.ANY)
GRANT = 12 * 1024 * 1024


class Dims:
    def __init__(self, groups, per_group, bs, bins, cycle):
        self.groups, self.per_group, self.bs = groups, per_group, bs
        self.bins, self.cycle = bins, cycle
        self.half = groups // 2 * per_group * bs
        self.rows = groups * bs
        self.slots = groups * per_group * per_group
        self.whole = cycle == 2 * HP and bins == cycle

    def at(self, j, s):
        return (j * self.per_group + s) * self.bs + (IDX if j >= self.groups // 2 else 0)


def ring_place(panel, cycle):
    return jnp.where(panel % 2 == 0, panel // 2, cycle - 1 - panel // 2)


def panel_number(dims, distance):
    me = lax.axis_index("rows").astype(jnp.int32)
    if not dims.whole:
        return (me + distance + dims.cycle) % dims.cycle
    place = (ring_place(me, dims.cycle) + distance + dims.cycle) % dims.cycle
    return jnp.where(place < dims.cycle // 2, 2 * place, 2 * (dims.cycle - 1 - place) + 1)


def first_bin(dims):
    me = lax.axis_index("rows").astype(jnp.int32)
    return (me - 2 * HP + 2 * dims.cycle) % dims.cycle


def stretch(tile, rows):
    return jnp.concatenate([tile] * (rows // 16), axis=0)


def prep_kernel(dims, blocks_ref, a_ref, b_ref, sems):
    me = lax.axis_index("cols").astype(jnp.int32)
    span = dims.per_group * dims.bs
    copies = []
    for j in range(dims.groups):
        at = j * span
        ref, start = (a_ref, at) if at < dims.half else (b_ref, at - dims.half)
        copy = pltpu.make_async_copy(
            blocks_ref.at[pl.ds((me ^ j) * span, span)], ref.at[start : start + span], sems.at[j]
        )
        copy.start()
        copies.append(copy)
    for copy in copies:
        copy.wait()


def number_kernel(dims, *refs):
    refs = list(refs)
    names = take(refs, dims.groups)
    a_ref, b_ref, full_ref, a_out, b_out, tile_ref, cols_ref, sems = refs
    copies = []
    for j in range(dims.groups):
        copies.append(pltpu.make_async_copy(names[j], cols_ref.at[j], sems.at[j]))
        copies[-1].start()
    half = dims.half
    for ref, out_ref, at in ((a_ref, a_out, 0), (b_ref, b_out, half + IDX)):
        value = ref[...]
        out_ref[0:half, :] = value
        full_ref[at : at + half, :] = value
    me = lax.axis_index("cols").astype(jnp.int32)
    line = lax.broadcasted_iota(jnp.int32, (IDX, 128), 0)
    lane = lax.broadcasted_iota(jnp.int32, (IDX, 128), 1)
    tile = jnp.zeros((IDX, 128), jnp.int32)
    for copy in copies:
        copy.wait()
    for j in range(dims.groups):
        row = jnp.zeros((IDX, 128), jnp.int32)
        for r in range(dims.groups):
            for s in range(dims.per_group):
                row = jnp.where(lane == r * dims.per_group + s, cols_ref[j, s, 0, me ^ j ^ r], row)
        tile = jnp.where(line == j, row, tile)
    numbers = (tile // dims.groups).astype(jnp.float32).astype(jnp.bfloat16)
    tile_ref[...] = numbers
    for ref in (a_out, b_out):
        ref[half : half + IDX, :] = numbers
    for at in (half, 2 * half + IDX):
        full_ref[at : at + IDX, :] = numbers


def accumulate(dims, pieces, left, lp_ref, d_ref, emit):
    groups, per_group, bs, bins = dims.groups, dims.per_group, dims.bs, dims.bins
    depth = dims.rows
    lrows = [ref[dims.half : dims.half + 16, :].astype(jnp.float32)[0:1, :] for ref in left]
    for n, (distance, *_) in enumerate(pieces):
        number = panel_number(dims, distance).astype(jnp.float32)
        for j in range(groups):
            hits = jnp.where(lrows[j] == number, 1.0, 0.0)
            for m in range(groups):
                total = None
                for t in range(per_group):
                    at = dims.at(m ^ j, t)
                    lane = (m ^ j) * per_group + t
                    hit = jnp.broadcast_to(hits[:, lane : lane + 1], (16, 128)).astype(jnp.bfloat16)
                    term = left[j][at : at + bs, :] * stretch(hit, bs)
                    total = term if total is None else total + term
                lp_ref[m * bs : (m + 1) * bs, n * depth + j * bs : n * depth + (j + 1) * bs] = total
    rows_of = []
    for *_, ref, at in pieces:
        row = ref[at : at + 16, :].astype(jnp.float32)[0:1, :]
        if dims.bins < dims.cycle:
            row = row - first_bin(dims).astype(jnp.float32)
            row = jnp.where(row < 0, row + float(dims.cycle), row)
        rows_of.append(row)
    for first in range(0, bins, 2):
        chunk = range(first, min(first + 2, bins))
        for n, (_, a_ref, b_ref, _, _) in enumerate(pieces):
            for b in chunk:
                hits = jnp.where(rows_of[n] == float(b), 1.0, 0.0)
                for j in range(groups):
                    total = None
                    for s in range(per_group):
                        ref, start = a_ref, dims.at(j, s)
                        if b_ref is not None and j >= groups // 2:
                            ref, start = b_ref, start - dims.half - IDX
                        lane = j * per_group + s
                        hit = jnp.broadcast_to(hits[:, lane : lane + 1], (16, 128)).astype(jnp.bfloat16)
                        term = ref[start : start + bs, :] * stretch(hit, bs)
                        total = term if total is None else total + term
                    d_ref[
                        n * depth + j * bs : n * depth + (j + 1) * bs, b * bs : (b + 1) * bs
                    ] = total
        lo, hi = first * bs, (first + len(chunk)) * bs
        emit(lo, hi, jnp.dot(lp_ref[...], d_ref[:, lo:hi], preferred_element_type=jnp.float32))


def take(refs, count):
    return [refs.pop(0) for _ in range(count)]


def take_pieces(dims, refs, layout):
    pieces = []
    for distance, two, where in layout:
        a_ref = refs.pop(0)
        b_ref = refs.pop(0) if two else None
        if where == "far":
            source, at = refs.pop(0), 0
        else:
            source, at = (b_ref if where == "b" else a_ref), dims.half
        pieces.append((distance, a_ref, b_ref, source, at))
    return pieces


def step_kernel(dims, layout, with_acc, blank_rows, tiles, *refs):
    refs = list(refs)
    left = take(refs, dims.groups)
    pieces = take_pieces(dims, refs, layout)
    tile_refs = take(refs, len(tiles))
    acc_ref = None
    if with_acc:
        acc_ref, _ = take(refs, 2)
    out_ref, zero_ref = take(refs, 2)
    index_refs = take(refs, 3) if tiles else None
    lp_ref, d_ref, blank_ref, sems = take(refs, 4)
    blank_ref[...] = jnp.zeros_like(blank_ref)
    copies = []
    for i in blank_rows:
        copy = pltpu.make_async_copy(blank_ref, zero_ref.at[i, dims.bins : dims.slots], sems.at[i])
        copy.start()
        copies.append(copy)
    if tiles:
        wide_ref, count_ref = refs
        index_work(dims, tiles, tile_refs, wide_ref, *index_refs, count_ref)

    def emit(lo, hi, value):
        out_ref[:, lo:hi] = value if acc_ref is None else acc_ref[:, lo:hi] + value

    accumulate(dims, pieces, left, lp_ref, d_ref, emit)
    for copy in copies:
        copy.wait()


def last_kernel(dims, layout, *refs):
    refs = list(refs)
    left = take(refs, dims.groups)
    pieces = take_pieces(dims, refs, layout)
    acc_ref, slot_ref, _, out_ref, lp_ref, d_ref, stage_ref, sems = refs
    groups, bs, bins = dims.groups, dims.bs, dims.bins
    me = lax.axis_index("cols").astype(jnp.int32)
    copies = []

    def emit(lo, hi, value):
        value = (acc_ref[:, lo:hi] + value).astype(jnp.bfloat16)
        for b in range(lo // bs, hi // bs):
            for m in range(groups):
                k = m * bins + b
                at = b * bs - lo
                stage_ref[k] = value[m * bs : (m + 1) * bs, at : at + bs]
                copy = pltpu.make_async_copy(
                    stage_ref.at[k], out_ref.at[m ^ me, slot_ref[k]], sems.at[k]
                )
                copy.start()
                copies.append(copy)

    accumulate(dims, pieces, left, lp_ref, d_ref, emit)
    for copy in copies:
        copy.wait()


def index_work(dims, tiles, tile_refs, wide_ref, slot_ref, cols_ref, start_ref, count_ref):
    groups, per_group, bins, cycle = dims.groups, dims.per_group, dims.bins, dims.cycle
    p = lax.axis_index("rows").astype(jnp.int32)
    c = lax.axis_index("cols").astype(jnp.int32)
    for (n, at), ref in zip(tiles, tile_refs):
        tile = ref[at : at + IDX, :].astype(jnp.float32).astype(jnp.int32)
        for j in range(groups):
            wide_ref[j * cycle + n : j * cycle + n + 1, :] = tile[j : j + 1]
    held = [wide_ref[j * cycle : (j + 1) * cycle, :] for j in range(groups)]
    bit = jnp.int32(1) << held[0]
    found = []
    for j in range(groups):
        lanes = range(j * per_group, (j + 1) * per_group)
        union = functools.reduce(jnp.bitwise_or, [bit[:, k : k + 1] for k in lanes])
        union = jnp.broadcast_to(union, (cycle, 128))
        look = jnp.zeros((cycle, 128), jnp.int32)
        for n in range(cycle):
            row = jnp.broadcast_to(union[n : n + 1, :], (cycle, 128))
            look = jnp.where(held[j] == panel_number(dims, n), row, look)
        found.append(look)
    panels = panel_number(dims, lax.broadcasted_iota(jnp.int32, (cycle, 1), 0))
    total = jnp.zeros((cycle, 1), jnp.int32)
    for m in range(groups):
        picks = []
        for j in range(groups):
            for t in range(per_group):
                lane = (m ^ j) * per_group + t
                picks.append(found[j][:, lane : lane + 1])
        bits = functools.reduce(jnp.bitwise_or, picks)
        for b in range(bins):
            total = total + ((bits >> b) & 1)
        mine = bits[0, 0]
        count = jnp.int32(0)
        for b in range(bins):
            count = count + ((mine >> b) & 1)
        count_ref[m ^ c] = count
        used = jnp.int32(0)
        for b in range(bins):
            one = (mine >> b) & 1
            slot = jnp.where(one == 1, used, count + b - used)
            slot_ref[m * bins + b] = slot
            cols_ref[m ^ c, 0, slot] = jnp.where(one == 1, b * groups + c, -1)
            used = used + one
    earlier = jnp.sum(jnp.where(panels < p, total, 0))
    for i in range(groups):
        start_ref[0, i] = earlier
        earlier = earlier + count_ref[i]
        for o in range(bins, dims.slots):
            cols_ref[i, 0, o] = -1


def flat(panels):
    layout, arrays = [], []
    for distance, first, second, where in panels:
        two = second is not None
        layout.append((distance, two, where if isinstance(where, str) else "far"))
        arrays += [first] + [second] * two + [where] * (not isinstance(where, str))
    return layout, arrays


def scratch_of(dims, panels):
    depth = dims.rows * len(panels)
    return [
        pltpu.VMEM((dims.rows, depth), jnp.bfloat16),
        pltpu.VMEM((depth, dims.bins * dims.bs), jnp.bfloat16),
    ]


def cost_of(dims, panels):
    flops = 2 * dims.rows * dims.rows * len(panels) * dims.bins * dims.bs
    return pl.CostEstimate(flops=flops, bytes_accessed=4_000_000, transcendentals=0)


def call_step(dims, left, panels, carry, blank_rows, tiles=()):
    layout, arrays = flat(panels)
    args = [*left, *arrays, *(array for _, array, _ in tiles)]
    specs = [VMEM] * len(args)
    aliases = {}
    if carry is not None:
        aliases = {len(args): 0, len(args) + 1: 1}
        args += carry
        specs += [VMEM, ANY]
    shapes = [
        jax.ShapeDtypeStruct((dims.rows, dims.bins * dims.bs), jnp.float32),
        jax.ShapeDtypeStruct((dims.groups, dims.slots, dims.bs, dims.bs), jnp.bfloat16),
    ]
    out_specs = [VMEM, ANY]
    scratch = scratch_of(dims, panels) + [
        pltpu.VMEM((dims.slots - dims.bins, dims.bs, dims.bs), jnp.bfloat16),
        pltpu.SemaphoreType.DMA((dims.groups,)),
    ]
    if tiles:
        shapes += [
            jax.ShapeDtypeStruct((dims.groups * dims.bins,), jnp.int32),
            jax.ShapeDtypeStruct((dims.groups, 1, dims.slots), jnp.int32),
            jax.ShapeDtypeStruct((1, dims.groups), jnp.int32),
        ]
        out_specs += [SMEM] * 3
        scratch += [
            pltpu.VMEM((dims.groups * dims.cycle, 128), jnp.int32),
            pltpu.SMEM((dims.groups,), jnp.int32),
        ]
    marks = tuple((n, at) for n, _, at in tiles)
    return pl.pallas_call(
        functools.partial(step_kernel, dims, layout, carry is not None, tuple(blank_rows), marks),
        out_shape=shapes,
        in_specs=specs,
        out_specs=out_specs,
        scratch_shapes=scratch,
        input_output_aliases=aliases,
        compiler_params=pltpu.CompilerParams(vmem_limit_bytes=GRANT),
        cost_estimate=cost_of(dims, panels),
    )(*args)


def call_last(dims, left, panels, acc, slots, empty):
    layout, arrays = flat(panels)
    args = [*left, *arrays, acc, slots, empty]
    return pl.pallas_call(
        functools.partial(last_kernel, dims, layout),
        out_shape=jax.ShapeDtypeStruct(empty.shape, empty.dtype),
        in_specs=[VMEM] * (len(args) - 2) + [SMEM, ANY],
        out_specs=ANY,
        scratch_shapes=scratch_of(dims, panels)
        + [
            pltpu.VMEM((dims.groups * dims.bins, dims.bs, dims.bs), jnp.bfloat16),
            pltpu.SemaphoreType.DMA((dims.groups * dims.bins,)),
        ],
        input_output_aliases={len(args) - 1: 0},
        compiler_params=pltpu.CompilerParams(vmem_limit_bytes=GRANT),
        cost_estimate=cost_of(dims, panels),
    )(*args)


def xor_move(value, axis, bit):
    return lax.ppermute(value, axis, [(i, i ^ bit) for i in range(lax.axis_size(axis))])


def shifted(value, axis, distance):
    size = lax.axis_size(axis)
    return lax.ppermute(value, axis, [((i - distance) % size, i) for i in range(size)])


def ring_moves(cycle):
    ring = [2 * k for k in range(cycle // 2)] + [2 * k + 1 for k in reversed(range(cycle // 2))]
    up = [(ring[k], ring[(k + 1) % cycle]) for k in range(cycle)]
    return up, [(b, a) for a, b in up]


def one_of(values, wanted):
    return jnp.any(values[..., None] == wanted, axis=-2)


def window_index(dims, left, window):
    groups, per_group, bins, cycle = dims.groups, dims.per_group, dims.bins, dims.cycle
    p = lax.axis_index("rows").astype(jnp.int32)
    c = lax.axis_index("cols").astype(jnp.int32)
    lanes = jnp.arange(groups, dtype=jnp.int32)

    def numbers_of(array):
        numbers = array[dims.half, : groups * per_group].astype(jnp.int32)
        return numbers.reshape(groups, per_group)

    held = jnp.stack(
        [numbers_of(left[j])[jnp.array([m ^ j for m in range(groups)])] for j in range(groups)], axis=1
    )
    lrel = (held - (p - HP)) % cycle
    zero = (p - 2 * HP) % cycle if bins < cycle else jnp.int32(0)
    bin_ids = jnp.arange(bins, dtype=jnp.int32)
    bin_abs = (zero + bin_ids) % cycle
    has = jnp.stack([one_of((numbers_of(w) - zero) % cycle, bin_ids) for w in window])
    uses = one_of(lrel, jnp.arange(2 * HP, dtype=jnp.int32))
    hits = jnp.any(uses.transpose(0, 2, 1)[..., None] & has[None], axis=(1, 2))
    counts = jnp.sum(hits.astype(jnp.int32), axis=-1)
    all_totals = lax.all_gather(jnp.sum(counts).reshape(1), "rows", axis=0, tiled=True)
    earlier = jnp.sum(jnp.where(jnp.arange(cycle, dtype=jnp.int32) < p, all_totals, 0))
    lower = bin_abs[:, None] < bin_abs[None, :]
    rank_in = jnp.sum((hits[:, :, None] & lower[None]).astype(jnp.int32), axis=1)
    rank_out = jnp.sum((~hits[:, :, None] & lower[None]).astype(jnp.int32), axis=1)
    slots = jnp.where(hits, rank_in, counts[:, None] + rank_out)
    at_slot = hits[:, None, :] & (slots[:, None, :] == jnp.arange(dims.slots, dtype=jnp.int32)[:, None])
    columns = jnp.sum(jnp.where(at_slot, bin_abs * groups + c + 1, 0), axis=-1) - 1
    pick = (lanes[:, None] ^ c) == lanes[None, :]
    columns = jnp.sum(jnp.where(pick[:, :, None], columns[None], 0), axis=1)
    before = (lanes[None, :] ^ c) < lanes[:, None]
    starts = earlier + jnp.sum(jnp.where(before, counts[None, :], 0), axis=1)
    return slots.reshape(-1), columns[:, None].astype(jnp.int32), starts[:, None].astype(jnp.int32)


def on_device(blocks, block_cols):
    panel_rows, _, per_group, bs, _ = blocks.shape
    groups = lax.axis_size("cols")
    cycle = lax.axis_size("rows")
    if groups != 4 or panel_rows != groups or cycle > 256 or cycle < 2 * HP:
        raise ValueError("unsupported sizes")
    dims = Dims(groups, per_group, bs, min(cycle, 4 * HP - 1), cycle)

    def payload(rows):
        return jax.ShapeDtypeStruct((rows, bs), jnp.bfloat16)

    params = pltpu.CompilerParams(vmem_limit_bytes=GRANT)
    cols = [block_cols] + [xor_move(block_cols, "cols", j) for j in range(1, groups)]
    cols = [jnp.transpose(x, (2, 1, 0)) for x in cols]
    cols[0] = pltpu.with_memory_space_constraint(cols[0], pltpu.HBM)
    flat_blocks = pltpu.with_memory_space_constraint(blocks.reshape(-1, bs), pltpu.HBM)
    bare_a, bare_b = pl.pallas_call(
        functools.partial(prep_kernel, dims),
        out_shape=[payload(dims.half)] * 2,
        in_specs=[ANY],
        out_specs=[VMEM] * 2,
        scratch_shapes=[pltpu.SemaphoreType.DMA((groups,))],
        compiler_params=params,
        name="prep",
    )(flat_blocks)
    own, own_a, own_b, tile = pl.pallas_call(
        functools.partial(number_kernel, dims),
        out_shape=[payload(2 * dims.half + 2 * IDX)] + [payload(dims.half + IDX)] * 2 + [payload(IDX)],
        in_specs=[ANY] * groups + [VMEM] * 2,
        out_specs=[VMEM] * 4,
        scratch_shapes=[
            pltpu.SMEM((groups, per_group, 1, groups), jnp.int32),
            pltpu.SemaphoreType.DMA((groups,)),
        ],
        compiler_params=params,
        name="numbers",
    )(*cols, bare_a, bare_b)

    if dims.whole:
        up, down = ring_moves(cycle)
        pa, pb, qa, qb = [bare_a], [own_b], [own_a], [bare_b]
        for k in range(1, HP + 1):
            pa.append(lax.ppermute(pa[-1], "rows", up))
            qb.append(lax.ppermute(qb[-1], "rows", down))
            if k < HP:
                pb.append(lax.ppermute(pb[-1], "rows", up))
                qa.append(lax.ppermute(qa[-1], "rows", down))
    else:
        window = [own if k == 0 else shifted(own, "rows", -k) for k in range(-HP, HP)]
    left1 = xor_move(own, "cols", 1)
    left2 = xor_move(own, "cols", 2)
    left3 = xor_move(left2, "cols", 1)
    left = [own, left1, left2, left3]

    if dims.whole:
        far = lax.ppermute(tile, "rows", [(a, dict(up)[dict(up)[dict(up)[b]]]) for a, b in up])
        pairs = [[(-k, pa[k], pb[k], "b"), (k, qa[k], qb[k], "a")] for k in range(1, HP)]
        carry = call_step(dims, left, [(0, own, None, "a")] + pairs[0], None, [0, 1])
        carry = call_step(dims, left, pairs[1], carry, [2])
        tiles = [(0, tile, 0), (HP, far, 0)]
        for k in range(1, HP):
            tiles += [(cycle - k, pb[k], dims.half), (k, qa[k], dims.half)]
        acc, empty, slots, columns, starts = call_step(dims, left, pairs[2], carry, [3], tiles)
        starts = starts.reshape(groups, 1)
        final = [(HP, pa[HP], qb[HP], far)]
    else:
        slots, columns, starts = window_index(dims, left, window)
        carry = call_step(dims, left, [(0, own, None, "a")], None, range(groups))
        pairs = [(k, window[k + HP], None, "a") for k in range(-HP, HP) if k]
        for k in range(0, len(pairs) - 1, 2):
            carry = call_step(dims, left, pairs[k : k + 2], carry, [])
        final = pairs[-1:]
        acc, empty = carry
    out = call_last(dims, left, final, acc, slots, empty)
    return out[:, None], columns, starts


def solution(mesh):
    in_specs = (P("rows", "cols", None, None, None), P("rows", "cols", None))
    out_specs = (P("rows", "cols", None, None, None), P("rows", "cols", None), P("rows", "cols"))

    return jax.shard_map(on_device, mesh=mesh, in_specs=in_specs, out_specs=out_specs, check_vma=False)
```

```python
import functools

import jax
import jax.numpy as jnp
from jax import lax
from jax.experimental import pallas as pl
from jax.experimental.pallas import tpu as pltpu
from jax.sharding import PartitionSpec as P


HP = 4
IDX = 16


VMEM = pl.BlockSpec(memory_space=pltpu.VMEM)
SMEM = pl.BlockSpec(memory_space=pltpu.SMEM)
ANY = pl.BlockSpec(memory_space=pl.ANY)
GRANT = 12 * 1024 * 1024


class Dims:
    def __init__(self, groups, per_group, bs, bins, cycle):
        self.groups, self.per_group, self.bs = groups, per_group, bs
        self.bins, self.cycle = bins, cycle
        self.half = groups // 2 * per_group * bs
        self.rows = groups * bs
        self.slots = groups * per_group * per_group
        self.whole = cycle == 2 * HP and bins == cycle

    def at(self, j, s):
        return (j * self.per_group + s) * self.bs + (IDX if j >= self.groups // 2 else 0)


def ring_place(panel, cycle):
    return jnp.where(panel % 2 == 0, panel // 2, cycle - 1 - panel // 2)


def panel_number(dims, distance):
    me = lax.axis_index("rows").astype(jnp.int32)
    if not dims.whole:
        return (me + distance + dims.cycle) % dims.cycle
    place = (ring_place(me, dims.cycle) + distance + dims.cycle) % dims.cycle
    return jnp.where(place < dims.cycle // 2, 2 * place, 2 * (dims.cycle - 1 - place) + 1)


def first_bin(dims):
    me = lax.axis_index("rows").astype(jnp.int32)
    return (me - 2 * HP + 2 * dims.cycle) % dims.cycle


def stretch(tile, rows):
    return jnp.concatenate([tile] * (rows // 16), axis=0)


def prep_kernel(dims, blocks_ref, a_ref, b_ref, sems):
    me = lax.axis_index("cols").astype(jnp.int32)
    span = dims.per_group * dims.bs
    copies = []
    for j in range(dims.groups):
        at = j * span
        ref, start = (a_ref, at) if at < dims.half else (b_ref, at - dims.half)
        copy = pltpu.make_async_copy(
            blocks_ref.at[pl.ds((me ^ j) * span, span)], ref.at[start : start + span], sems.at[j]
        )
        copy.start()
        copies.append(copy)
    for copy in copies:
        copy.wait()


def number_kernel(dims, *refs):
    refs = list(refs)
    names = take(refs, dims.groups)
    a_ref, b_ref, full_ref, a_out, b_out, tile_ref, cols_ref, sems = refs
    copies = []
    for j in range(dims.groups):
        copies.append(pltpu.make_async_copy(names[j], cols_ref.at[j], sems.at[j]))
        copies[-1].start()
    half = dims.half
    for ref, out_ref, at in ((a_ref, a_out, 0), (b_ref, b_out, half + IDX)):
        value = ref[...]
        out_ref[0:half, :] = value
        full_ref[at : at + half, :] = value
    me = lax.axis_index("cols").astype(jnp.int32)
    line = lax.broadcasted_iota(jnp.int32, (IDX, 128), 0)
    lane = lax.broadcasted_iota(jnp.int32, (IDX, 128), 1)
    tile = jnp.zeros((IDX, 128), jnp.int32)
    for copy in copies:
        copy.wait()
    for j in range(dims.groups):
        row = jnp.zeros((IDX, 128), jnp.int32)
        for r in range(dims.groups):
            for s in range(dims.per_group):
                row = jnp.where(lane == r * dims.per_group + s, cols_ref[j, s, 0, me ^ j ^ r], row)
        tile = jnp.where(line == j, row, tile)
    numbers = (tile // dims.groups).astype(jnp.float32).astype(jnp.bfloat16)
    tile_ref[...] = numbers
    for ref in (a_out, b_out):
        ref[half : half + IDX, :] = numbers
    for at in (half, 2 * half + IDX):
        full_ref[at : at + IDX, :] = numbers


def accumulate(dims, pieces, left, lp_ref, d_ref, emit):
    groups, per_group, bs, bins = dims.groups, dims.per_group, dims.bs, dims.bins
    depth = dims.rows
    lrows = [ref[dims.half : dims.half + 16, :].astype(jnp.float32)[0:1, :] for ref in left]
    for n, (distance, *_) in enumerate(pieces):
        number = panel_number(dims, distance).astype(jnp.float32)
        for j in range(groups):
            hits = jnp.where(lrows[j] == number, 1.0, 0.0)
            for m in range(groups):
                total = None
                for t in range(per_group):
                    at = dims.at(m ^ j, t)
                    lane = (m ^ j) * per_group + t
                    hit = jnp.broadcast_to(hits[:, lane : lane + 1], (16, 128)).astype(jnp.bfloat16)
                    term = left[j][at : at + bs, :] * stretch(hit, bs)
                    total = term if total is None else total + term
                lp_ref[m * bs : (m + 1) * bs, n * depth + j * bs : n * depth + (j + 1) * bs] = total
    rows_of = []
    for *_, ref, at in pieces:
        row = ref[at : at + 16, :].astype(jnp.float32)[0:1, :]
        if dims.bins < dims.cycle:
            row = row - first_bin(dims).astype(jnp.float32)
            row = jnp.where(row < 0, row + float(dims.cycle), row)
        rows_of.append(row)
    for first in range(0, bins, 2):
        chunk = range(first, min(first + 2, bins))
        for n, (_, a_ref, b_ref, _, _) in enumerate(pieces):
            for b in chunk:
                hits = jnp.where(rows_of[n] == float(b), 1.0, 0.0)
                for j in range(groups):
                    total = None
                    for s in range(per_group):
                        ref, start = a_ref, dims.at(j, s)
                        if b_ref is not None and j >= groups // 2:
                            ref, start = b_ref, start - dims.half - IDX
                        lane = j * per_group + s
                        hit = jnp.broadcast_to(hits[:, lane : lane + 1], (16, 128)).astype(jnp.bfloat16)
                        term = ref[start : start + bs, :] * stretch(hit, bs)
                        total = term if total is None else total + term
                    d_ref[
                        n * depth + j * bs : n * depth + (j + 1) * bs, b * bs : (b + 1) * bs
                    ] = total
        lo, hi = first * bs, (first + len(chunk)) * bs
        emit(lo, hi, jnp.dot(lp_ref[...], d_ref[:, lo:hi], preferred_element_type=jnp.float32))


def take(refs, count):
    return [refs.pop(0) for _ in range(count)]


def take_pieces(dims, refs, layout):
    pieces = []
    for distance, two, where in layout:
        a_ref = refs.pop(0)
        b_ref = refs.pop(0) if two else None
        if where == "far":
            source, at = refs.pop(0), 0
        else:
            source, at = (b_ref if where == "b" else a_ref), dims.half
        pieces.append((distance, a_ref, b_ref, source, at))
    return pieces


def zero_kernel(dims, out_ref, blank_ref, sems):
    per = blank_ref.shape[0]
    blank_ref[...] = jnp.zeros_like(blank_ref)
    copies = []
    for i in range(dims.groups):
        for first in range(dims.bins, dims.slots, per):
            copies.append(
                pltpu.make_async_copy(blank_ref, out_ref.at[i, first : first + per], sems.at[len(copies)])
            )
            copies[-1].start()
    for copy in copies:
        copy.wait()


def step_kernel(dims, layout, with_acc, tiles, *refs):
    refs = list(refs)
    left = take(refs, dims.groups)
    pieces = take_pieces(dims, refs, layout)
    tile_refs = take(refs, len(tiles))
    acc_ref = refs.pop(0) if with_acc else None
    out_ref = refs.pop(0)
    index_refs = take(refs, 3) if tiles else None
    lp_ref, d_ref = take(refs, 2)
    if tiles:
        wide_ref, count_ref = refs
        index_work(dims, tiles, tile_refs, wide_ref, *index_refs, count_ref)

    def emit(lo, hi, value):
        out_ref[:, lo:hi] = value if acc_ref is None else acc_ref[:, lo:hi] + value

    accumulate(dims, pieces, left, lp_ref, d_ref, emit)


def last_kernel(dims, layout, *refs):
    refs = list(refs)
    left = take(refs, dims.groups)
    pieces = take_pieces(dims, refs, layout)
    acc_ref, slot_ref, _, out_ref, lp_ref, d_ref, stage_ref, sems = refs
    groups, bs, bins = dims.groups, dims.bs, dims.bins
    me = lax.axis_index("cols").astype(jnp.int32)
    copies = []

    def emit(lo, hi, value):
        value = (acc_ref[:, lo:hi] + value).astype(jnp.bfloat16)
        for b in range(lo // bs, hi // bs):
            for m in range(groups):
                k = m * bins + b
                at = b * bs - lo
                stage_ref[k] = value[m * bs : (m + 1) * bs, at : at + bs]
                copy = pltpu.make_async_copy(
                    stage_ref.at[k], out_ref.at[m ^ me, slot_ref[k]], sems.at[k]
                )
                copy.start()
                copies.append(copy)

    accumulate(dims, pieces, left, lp_ref, d_ref, emit)
    for copy in copies:
        copy.wait()


def index_work(dims, tiles, tile_refs, wide_ref, slot_ref, cols_ref, start_ref, count_ref):
    groups, per_group, bins, cycle = dims.groups, dims.per_group, dims.bins, dims.cycle
    p = lax.axis_index("rows").astype(jnp.int32)
    c = lax.axis_index("cols").astype(jnp.int32)
    for (n, at), ref in zip(tiles, tile_refs):
        tile = ref[at : at + IDX, :].astype(jnp.float32).astype(jnp.int32)
        for j in range(groups):
            wide_ref[j * cycle + n : j * cycle + n + 1, :] = tile[j : j + 1]
    held = [wide_ref[j * cycle : (j + 1) * cycle, :] for j in range(groups)]
    bit = jnp.int32(1) << held[0]
    found = []
    for j in range(groups):
        lanes = range(j * per_group, (j + 1) * per_group)
        union = functools.reduce(jnp.bitwise_or, [bit[:, k : k + 1] for k in lanes])
        union = jnp.broadcast_to(union, (cycle, 128))
        look = jnp.zeros((cycle, 128), jnp.int32)
        for n in range(cycle):
            row = jnp.broadcast_to(union[n : n + 1, :], (cycle, 128))
            look = jnp.where(held[j] == panel_number(dims, n), row, look)
        found.append(look)
    panels = panel_number(dims, lax.broadcasted_iota(jnp.int32, (cycle, 1), 0))
    total = jnp.zeros((cycle, 1), jnp.int32)
    for m in range(groups):
        picks = []
        for j in range(groups):
            for t in range(per_group):
                lane = (m ^ j) * per_group + t
                picks.append(found[j][:, lane : lane + 1])
        bits = functools.reduce(jnp.bitwise_or, picks)
        for b in range(bins):
            total = total + ((bits >> b) & 1)
        mine = bits[0, 0]
        count = jnp.int32(0)
        for b in range(bins):
            count = count + ((mine >> b) & 1)
        count_ref[m ^ c] = count
        used = jnp.int32(0)
        for b in range(bins):
            one = (mine >> b) & 1
            slot = jnp.where(one == 1, used, count + b - used)
            slot_ref[m * bins + b] = slot
            cols_ref[m ^ c, 0, slot] = jnp.where(one == 1, b * groups + c, -1)
            used = used + one
    earlier = jnp.sum(jnp.where(panels < p, total, 0))
    for i in range(groups):
        start_ref[0, i] = earlier
        earlier = earlier + count_ref[i]
        for o in range(bins, dims.slots):
            cols_ref[i, 0, o] = -1


def flat(panels):
    layout, arrays = [], []
    for distance, first, second, where in panels:
        two = second is not None
        layout.append((distance, two, where if isinstance(where, str) else "far"))
        arrays += [first] + [second] * two + [where] * (not isinstance(where, str))
    return layout, arrays


def scratch_of(dims, panels):
    depth = dims.rows * len(panels)
    return [
        pltpu.VMEM((dims.rows, depth), jnp.bfloat16),
        pltpu.VMEM((depth, dims.bins * dims.bs), jnp.bfloat16),
    ]


def cost_of(dims, panels):
    flops = 2 * dims.rows * dims.rows * len(panels) * dims.bins * dims.bs
    return pl.CostEstimate(flops=flops, bytes_accessed=4_000_000, transcendentals=0)


def call_zero(dims):
    count = dims.slots - dims.bins
    per = max(n for n in range(1, 5) if count % n == 0)
    return pl.pallas_call(
        functools.partial(zero_kernel, dims),
        out_shape=jax.ShapeDtypeStruct((dims.groups, dims.slots, dims.bs, dims.bs), jnp.bfloat16),
        out_specs=ANY,
        scratch_shapes=[
            pltpu.VMEM((per, dims.bs, dims.bs), jnp.bfloat16),
            pltpu.SemaphoreType.DMA((dims.groups * count // per,)),
        ],
        compiler_params=pltpu.CompilerParams(vmem_limit_bytes=GRANT),
        name="zero",
    )()


def call_step(dims, left, panels, acc, tiles=()):
    layout, arrays = flat(panels)
    args = [*left, *arrays, *(array for _, array, _ in tiles)]
    aliases = {}
    if acc is not None:
        aliases = {len(args): 0}
        args.append(acc)
    shapes = [jax.ShapeDtypeStruct((dims.rows, dims.bins * dims.bs), jnp.float32)]
    out_specs = [VMEM]
    scratch = scratch_of(dims, panels)
    if tiles:
        shapes += [
            jax.ShapeDtypeStruct((dims.groups * dims.bins,), jnp.int32),
            jax.ShapeDtypeStruct((dims.groups, 1, dims.slots), jnp.int32),
            jax.ShapeDtypeStruct((1, dims.groups), jnp.int32),
        ]
        out_specs += [SMEM] * 3
        scratch += [
            pltpu.VMEM((dims.groups * dims.cycle, 128), jnp.int32),
            pltpu.SMEM((dims.groups,), jnp.int32),
        ]
    marks = tuple((n, at) for n, _, at in tiles)
    return pl.pallas_call(
        functools.partial(step_kernel, dims, layout, acc is not None, marks),
        out_shape=shapes,
        in_specs=[VMEM] * len(args),
        out_specs=out_specs,
        scratch_shapes=scratch,
        input_output_aliases=aliases,
        compiler_params=pltpu.CompilerParams(vmem_limit_bytes=GRANT),
        cost_estimate=cost_of(dims, panels),
    )(*args)


def call_last(dims, left, panels, acc, slots, empty):
    layout, arrays = flat(panels)
    args = [*left, *arrays, acc, slots, empty]
    return pl.pallas_call(
        functools.partial(last_kernel, dims, layout),
        out_shape=jax.ShapeDtypeStruct(empty.shape, empty.dtype),
        in_specs=[VMEM] * (len(args) - 2) + [SMEM, ANY],
        out_specs=ANY,
        scratch_shapes=scratch_of(dims, panels)
        + [
            pltpu.VMEM((dims.groups * dims.bins, dims.bs, dims.bs), jnp.bfloat16),
            pltpu.SemaphoreType.DMA((dims.groups * dims.bins,)),
        ],
        input_output_aliases={len(args) - 1: 0},
        compiler_params=pltpu.CompilerParams(vmem_limit_bytes=GRANT),
        cost_estimate=cost_of(dims, panels),
    )(*args)


def xor_move(value, axis, bit):
    return lax.ppermute(value, axis, [(i, i ^ bit) for i in range(lax.axis_size(axis))])


def shifted(value, axis, distance):
    size = lax.axis_size(axis)
    return lax.ppermute(value, axis, [((i - distance) % size, i) for i in range(size)])


def ring_moves(cycle):
    ring = [2 * k for k in range(cycle // 2)] + [2 * k + 1 for k in reversed(range(cycle // 2))]
    up = [(ring[k], ring[(k + 1) % cycle]) for k in range(cycle)]
    return up, [(b, a) for a, b in up]


def one_of(values, wanted):
    return jnp.any(values[..., None] == wanted, axis=-2)


def window_index(dims, left, window):
    groups, per_group, bins, cycle = dims.groups, dims.per_group, dims.bins, dims.cycle
    p = lax.axis_index("rows").astype(jnp.int32)
    c = lax.axis_index("cols").astype(jnp.int32)
    lanes = jnp.arange(groups, dtype=jnp.int32)

    def numbers_of(array):
        numbers = array[dims.half, : groups * per_group].astype(jnp.int32)
        return numbers.reshape(groups, per_group)

    held = jnp.stack(
        [numbers_of(left[j])[jnp.array([m ^ j for m in range(groups)])] for j in range(groups)], axis=1
    )
    lrel = (held - (p - HP)) % cycle
    zero = (p - 2 * HP) % cycle if bins < cycle else jnp.int32(0)
    bin_ids = jnp.arange(bins, dtype=jnp.int32)
    bin_abs = (zero + bin_ids) % cycle
    has = jnp.stack([one_of((numbers_of(w) - zero) % cycle, bin_ids) for w in window])
    uses = one_of(lrel, jnp.arange(2 * HP, dtype=jnp.int32))
    hits = jnp.any(uses.transpose(0, 2, 1)[..., None] & has[None], axis=(1, 2))
    counts = jnp.sum(hits.astype(jnp.int32), axis=-1)
    all_totals = lax.all_gather(jnp.sum(counts).reshape(1), "rows", axis=0, tiled=True)
    earlier = jnp.sum(jnp.where(jnp.arange(cycle, dtype=jnp.int32) < p, all_totals, 0))
    lower = bin_abs[:, None] < bin_abs[None, :]
    rank_in = jnp.sum((hits[:, :, None] & lower[None]).astype(jnp.int32), axis=1)
    rank_out = jnp.sum((~hits[:, :, None] & lower[None]).astype(jnp.int32), axis=1)
    slots = jnp.where(hits, rank_in, counts[:, None] + rank_out)
    at_slot = hits[:, None, :] & (slots[:, None, :] == jnp.arange(dims.slots, dtype=jnp.int32)[:, None])
    columns = jnp.sum(jnp.where(at_slot, bin_abs * groups + c + 1, 0), axis=-1) - 1
    pick = (lanes[:, None] ^ c) == lanes[None, :]
    columns = jnp.sum(jnp.where(pick[:, :, None], columns[None], 0), axis=1)
    before = (lanes[None, :] ^ c) < lanes[:, None]
    starts = earlier + jnp.sum(jnp.where(before, counts[None, :], 0), axis=1)
    return slots.reshape(-1), columns[:, None].astype(jnp.int32), starts[:, None].astype(jnp.int32)


def on_device(blocks, block_cols):
    panel_rows, _, per_group, bs, _ = blocks.shape
    groups = lax.axis_size("cols")
    cycle = lax.axis_size("rows")
    if groups != 4 or panel_rows != groups or cycle > 256 or cycle < 2 * HP:
        raise ValueError("unsupported sizes")
    dims = Dims(groups, per_group, bs, min(cycle, 4 * HP - 1), cycle)

    def payload(rows):
        return jax.ShapeDtypeStruct((rows, bs), jnp.bfloat16)

    params = pltpu.CompilerParams(vmem_limit_bytes=GRANT)
    cols = [block_cols] + [xor_move(block_cols, "cols", j) for j in range(1, groups)]
    cols = [jnp.transpose(x, (2, 1, 0)) for x in cols]
    cols[0] = pltpu.with_memory_space_constraint(cols[0], pltpu.HBM)
    flat_blocks = pltpu.with_memory_space_constraint(blocks.reshape(-1, bs), pltpu.HBM)
    bare_a, bare_b = pl.pallas_call(
        functools.partial(prep_kernel, dims),
        out_shape=[payload(dims.half)] * 2,
        in_specs=[ANY],
        out_specs=[VMEM] * 2,
        scratch_shapes=[pltpu.SemaphoreType.DMA((groups,))],
        compiler_params=params,
        name="prep",
    )(flat_blocks)
    own, own_a, own_b, tile = pl.pallas_call(
        functools.partial(number_kernel, dims),
        out_shape=[payload(2 * dims.half + 2 * IDX)] + [payload(dims.half + IDX)] * 2 + [payload(IDX)],
        in_specs=[ANY] * groups + [VMEM] * 2,
        out_specs=[VMEM] * 4,
        scratch_shapes=[
            pltpu.SMEM((groups, per_group, 1, groups), jnp.int32),
            pltpu.SemaphoreType.DMA((groups,)),
        ],
        compiler_params=params,
        name="numbers",
    )(*cols, bare_a, bare_b)

    if dims.whole:
        up, down = ring_moves(cycle)
        pa, pb, qa, qb = [bare_a], [own_b], [own_a], [bare_b]
        for k in range(1, HP + 1):
            pa.append(lax.ppermute(pa[-1], "rows", up))
            qb.append(lax.ppermute(qb[-1], "rows", down))
            if k < HP:
                pb.append(lax.ppermute(pb[-1], "rows", up))
                qa.append(lax.ppermute(qa[-1], "rows", down))
    else:
        window = [own if k == 0 else shifted(own, "rows", -k) for k in range(-HP, HP)]
    left1 = xor_move(own, "cols", 1)
    left2 = xor_move(own, "cols", 2)
    left3 = xor_move(left2, "cols", 1)
    left = [own, left1, left2, left3]

    if dims.whole:
        far = lax.ppermute(tile, "rows", [(a, dict(up)[dict(up)[dict(up)[b]]]) for a, b in up])
        pairs = [[(-k, pa[k], pb[k], "b"), (k, qa[k], qb[k], "a")] for k in range(1, HP)]
        acc = call_step(dims, left, [(0, own, None, "a")] + pairs[0], None)[0]
        acc = call_step(dims, left, pairs[1], acc)[0]
        tiles = [(0, tile, 0), (HP, far, 0)]
        for k in range(1, HP):
            tiles += [(cycle - k, pb[k], dims.half), (k, qa[k], dims.half)]
        acc, slots, columns, starts = call_step(dims, left, pairs[2], acc, tiles)
        starts = starts.reshape(groups, 1)
        final = [(HP, pa[HP], qb[HP], far)]
    else:
        slots, columns, starts = window_index(dims, left, window)
        acc = call_step(dims, left, [(0, own, None, "a")], None)[0]
        pairs = [(k, window[k + HP], None, "a") for k in range(-HP, HP) if k]
        for k in range(0, len(pairs) - 1, 2):
            acc = call_step(dims, left, pairs[k : k + 2], acc)[0]
        final = pairs[-1:]
    empty = call_zero(dims)
    out = call_last(dims, left, final, acc, slots, empty)
    return out[:, None], columns, starts


def solution(mesh):
    in_specs = (P("rows", "cols", None, None, None), P("rows", "cols", None))
    out_specs = (P("rows", "cols", None, None, None), P("rows", "cols", None), P("rows", "cols"))

    return jax.shard_map(on_device, mesh=mesh, in_specs=in_specs, out_specs=out_specs, check_vma=False)
```

```python
import functools

import jax
import jax.numpy as jnp
from jax import lax
from jax.experimental import pallas as pl
from jax.experimental.pallas import tpu as pltpu
from jax.sharding import PartitionSpec as P


HP = 4
IDX = 16


VMEM = pl.BlockSpec(memory_space=pltpu.VMEM)
SMEM = pl.BlockSpec(memory_space=pltpu.SMEM)
ANY = pl.BlockSpec(memory_space=pl.ANY)
GRANT = 12 * 1024 * 1024


class Dims:
    def __init__(self, groups, per_group, bs, bins, cycle):
        self.groups, self.per_group, self.bs = groups, per_group, bs
        self.bins, self.cycle = bins, cycle
        self.half = groups // 2 * per_group * bs
        self.rows = groups * bs
        self.slots = groups * per_group * per_group
        self.whole = cycle == 2 * HP and bins == cycle

    def at(self, j, s):
        return (j * self.per_group + s) * self.bs


def ring_place(panel, cycle):
    return jnp.where(panel % 2 == 0, panel // 2, cycle - 1 - panel // 2)


def panel_number(dims, distance):
    me = lax.axis_index("rows").astype(jnp.int32)
    if not dims.whole:
        return (me + distance + dims.cycle) % dims.cycle
    place = (ring_place(me, dims.cycle) + distance + dims.cycle) % dims.cycle
    return jnp.where(place < dims.cycle // 2, 2 * place, 2 * (dims.cycle - 1 - place) + 1)


def first_bin(dims):
    me = lax.axis_index("rows").astype(jnp.int32)
    return (me - 2 * HP + 2 * dims.cycle) % dims.cycle


def stretch(tile, rows):
    return jnp.concatenate([tile] * (rows // 16), axis=0)


def prep_kernel(dims, blocks_ref, full_ref, a_ref, b_ref, sems):
    me = lax.axis_index("cols").astype(jnp.int32)
    span = dims.per_group * dims.bs
    copies = []
    for j in range(dims.groups):
        at = j * span
        ref, start = (a_ref, at) if at < dims.half else (b_ref, at - dims.half)
        for k, (out_ref, first) in enumerate(((ref, start), (full_ref, at))):
            copy = pltpu.make_async_copy(
                blocks_ref.at[pl.ds((me ^ j) * span, span)], out_ref.at[first : first + span], sems.at[j, k]
            )
            copy.start()
            copies.append(copy)
    for copy in copies:
        copy.wait()


def number_kernel(dims, *refs):
    refs = list(refs)
    names = take(refs, dims.groups)
    a_ref, b_ref, a_out, b_out, tile_ref, cols_ref, sems = refs
    copies = []
    for j in range(dims.groups):
        copies.append(pltpu.make_async_copy(names[j], cols_ref.at[j], sems.at[j]))
        copies[-1].start()
    half = dims.half
    for ref, out_ref in ((a_ref, a_out), (b_ref, b_out)):
        out_ref[0:half, :] = ref[...]
    me = lax.axis_index("cols").astype(jnp.int32)
    line = lax.broadcasted_iota(jnp.int32, (IDX, 128), 0)
    lane = lax.broadcasted_iota(jnp.int32, (IDX, 128), 1)
    tile = jnp.zeros((IDX, 128), jnp.int32)
    for copy in copies:
        copy.wait()
    for j in range(dims.groups):
        row = jnp.zeros((IDX, 128), jnp.int32)
        for r in range(dims.groups):
            for s in range(dims.per_group):
                row = jnp.where(lane == r * dims.per_group + s, cols_ref[j, s, 0, me ^ j ^ r], row)
        tile = jnp.where(line == j, row, tile)
    numbers = (tile // dims.groups).astype(jnp.float32).astype(jnp.bfloat16)
    tile_ref[...] = numbers
    for ref in (a_out, b_out):
        ref[half : half + IDX, :] = numbers


def left_matrix(dims, distance, left, tile_ref, lp_ref, first):
    per_group, bs = dims.per_group, dims.bs
    numbers = tile_ref[...].astype(jnp.float32)
    hits = jnp.where(numbers == panel_number(dims, distance).astype(jnp.float32), 1.0, 0.0)
    for j in range(dims.groups):
        for m in range(dims.groups):
            total = None
            for t in range(per_group):
                at = dims.at(m ^ j, t)
                lane = (m ^ j) * per_group + t
                hit = jnp.broadcast_to(hits[j : j + 1, lane : lane + 1], (16, 128)).astype(jnp.bfloat16)
                term = left[j][at : at + bs, :] * stretch(hit, bs)
                total = term if total is None else total + term
            lp_ref[m * bs : (m + 1) * bs, first + j * bs : first + (j + 1) * bs] = total


def accumulate(dims, pieces, lp_ref, d_ref, emit):
    groups, per_group, bs, bins = dims.groups, dims.per_group, dims.bs, dims.bins
    depth = dims.rows
    rows_of = []
    for *_, ref, at in pieces:
        row = ref[at : at + 16, :].astype(jnp.float32)[0:1, :]
        if dims.bins < dims.cycle:
            row = row - first_bin(dims).astype(jnp.float32)
            row = jnp.where(row < 0, row + float(dims.cycle), row)
        rows_of.append(row)
    for first in range(0, bins, 2):
        chunk = range(first, min(first + 2, bins))
        for n, (_, a_ref, b_ref, _, _) in enumerate(pieces):
            for b in chunk:
                hits = jnp.where(rows_of[n] == float(b), 1.0, 0.0)
                for j in range(groups):
                    total = None
                    for s in range(per_group):
                        ref, start = a_ref, dims.at(j, s)
                        if b_ref is not None and j >= groups // 2:
                            ref, start = b_ref, start - dims.half
                        lane = j * per_group + s
                        hit = jnp.broadcast_to(hits[:, lane : lane + 1], (16, 128)).astype(jnp.bfloat16)
                        term = ref[start : start + bs, :] * stretch(hit, bs)
                        total = term if total is None else total + term
                    d_ref[
                        n * depth + j * bs : n * depth + (j + 1) * bs, b * bs : (b + 1) * bs
                    ] = total
        lo, hi = first * bs, (first + len(chunk)) * bs
        emit(lo, hi, jnp.dot(lp_ref[...], d_ref[:, lo:hi], preferred_element_type=jnp.float32))


def take(refs, count):
    return [refs.pop(0) for _ in range(count)]


def take_pieces(dims, refs, layout):
    pieces = []
    for distance, two, where in layout:
        a_ref = refs.pop(0)
        b_ref = refs.pop(0) if two else None
        if where == "far":
            source, at = refs.pop(0), 0
        else:
            source, at = (b_ref if where == "b" else a_ref), dims.half if two else 2 * dims.half
        pieces.append((distance, a_ref, b_ref, source, at))
    return pieces


def zero_kernel(dims, out_ref, blank_ref, sems):
    per = blank_ref.shape[0]
    blank_ref[...] = jnp.zeros_like(blank_ref)
    copies = []
    for i in range(dims.groups):
        for first in range(dims.bins, dims.slots, per):
            copies.append(
                pltpu.make_async_copy(blank_ref, out_ref.at[i, first : first + per], sems.at[len(copies)])
            )
            copies[-1].start()
    for copy in copies:
        copy.wait()


def step_kernel(dims, layout, with_acc, ahead, tiles, *refs):
    refs = list(refs)
    left = take(refs, dims.groups)
    tile_ref = refs.pop(0)
    pieces = take_pieces(dims, refs, layout)
    tile_refs = take(refs, len(tiles))
    acc_ref = refs.pop(0) if with_acc else None
    out_ref = refs.pop(0)
    ahead_ref = refs.pop(0) if ahead is not None else None
    index_refs = take(refs, 3) if tiles else None
    lp_ref, d_ref = take(refs, 2)
    copies = []
    if tiles:
        wide_ref, count_ref, slot_ref, cols_ref, start_ref, sems = refs
        index_work(dims, tiles, tile_refs, wide_ref, slot_ref, cols_ref, start_ref, count_ref)
        for k, (ref, out) in enumerate(zip((slot_ref, cols_ref, start_ref), index_refs)):
            copies.append(pltpu.make_async_copy(ref, out, sems.at[k]))
            copies[-1].start()

    def emit(lo, hi, value):
        out_ref[:, lo:hi] = value if acc_ref is None else acc_ref[:, lo:hi] + value

    for n, (distance, *_) in enumerate(pieces):
        left_matrix(dims, distance, left, tile_ref, lp_ref, n * dims.rows)
    accumulate(dims, pieces, lp_ref, d_ref, emit)
    if ahead is not None:
        left_matrix(dims, ahead, left, tile_ref, ahead_ref, 0)
    for copy in copies:
        copy.wait()


def last_kernel(dims, layout, *refs):
    refs = list(refs)
    pieces = take_pieces(dims, refs, layout)
    lp_ref, acc_ref, slots_ref, _, out_ref, d_ref, stage_ref, slot_ref, sems, sem = refs
    groups, bs, bins = dims.groups, dims.bs, dims.bins
    me = lax.axis_index("cols").astype(jnp.int32)
    slots = pltpu.make_async_copy(slots_ref, slot_ref, sem)
    slots.start()
    copies = []

    def emit(lo, hi, value):
        value = (acc_ref[:, lo:hi] + value).astype(jnp.bfloat16)
        if lo == 0:
            slots.wait()
        for b in range(lo // bs, hi // bs):
            for m in range(groups):
                k = m * bins + b
                at = b * bs - lo
                stage_ref[k] = value[m * bs : (m + 1) * bs, at : at + bs]
                copy = pltpu.make_async_copy(
                    stage_ref.at[k], out_ref.at[m ^ me, slot_ref[k]], sems.at[k]
                )
                copy.start()
                copies.append(copy)

    accumulate(dims, pieces, lp_ref, d_ref, emit)
    for copy in copies:
        copy.wait()


def index_work(dims, tiles, tile_refs, wide_ref, slot_ref, cols_ref, start_ref, count_ref):
    groups, per_group, bins, cycle = dims.groups, dims.per_group, dims.bins, dims.cycle
    p = lax.axis_index("rows").astype(jnp.int32)
    c = lax.axis_index("cols").astype(jnp.int32)
    for (n, at), ref in zip(tiles, tile_refs):
        tile = ref[at : at + IDX, :].astype(jnp.float32).astype(jnp.int32)
        for j in range(groups):
            wide_ref[j * cycle + n : j * cycle + n + 1, :] = tile[j : j + 1]
    held = [wide_ref[j * cycle : (j + 1) * cycle, :] for j in range(groups)]
    bit = jnp.int32(1) << held[0]
    found = []
    for j in range(groups):
        lanes = range(j * per_group, (j + 1) * per_group)
        union = functools.reduce(jnp.bitwise_or, [bit[:, k : k + 1] for k in lanes])
        union = jnp.broadcast_to(union, (cycle, 128))
        look = jnp.zeros((cycle, 128), jnp.int32)
        for n in range(cycle):
            row = jnp.broadcast_to(union[n : n + 1, :], (cycle, 128))
            look = jnp.where(held[j] == panel_number(dims, n), row, look)
        found.append(look)
    panels = panel_number(dims, lax.broadcasted_iota(jnp.int32, (cycle, 1), 0))
    total = jnp.zeros((cycle, 1), jnp.int32)
    for m in range(groups):
        picks = []
        for j in range(groups):
            for t in range(per_group):
                lane = (m ^ j) * per_group + t
                picks.append(found[j][:, lane : lane + 1])
        bits = functools.reduce(jnp.bitwise_or, picks)
        for b in range(bins):
            total = total + ((bits >> b) & 1)
        mine = bits[0, 0]
        count = jnp.int32(0)
        for b in range(bins):
            count = count + ((mine >> b) & 1)
        count_ref[m ^ c] = count
        used = jnp.int32(0)
        for b in range(bins):
            one = (mine >> b) & 1
            slot = jnp.where(one == 1, used, count + b - used)
            slot_ref[m * bins + b] = slot
            cols_ref[m ^ c, 0, slot] = jnp.where(one == 1, b * groups + c, -1)
            used = used + one
    earlier = jnp.sum(jnp.where(panels < p, total, 0))
    for i in range(groups):
        start_ref[0, i] = earlier
        earlier = earlier + count_ref[i]
        for o in range(bins, dims.slots):
            cols_ref[i, 0, o] = -1


def flat(panels):
    layout, arrays = [], []
    for distance, first, second, where in panels:
        two = second is not None
        layout.append((distance, two, where if isinstance(where, str) else "far"))
        arrays += [first] + [second] * two + [where] * (not isinstance(where, str))
    return layout, arrays


def scratch_of(dims, panels):
    depth = dims.rows * len(panels)
    return [
        pltpu.VMEM((dims.rows, depth), jnp.bfloat16),
        pltpu.VMEM((depth, dims.bins * dims.bs), jnp.bfloat16),
    ]


def cost_of(dims, panels):
    flops = 2 * dims.rows * dims.rows * len(panels) * dims.bins * dims.bs
    return pl.CostEstimate(flops=flops, bytes_accessed=4_000_000, transcendentals=0)


def call_zero(dims):
    count = dims.slots - dims.bins
    per = max(n for n in range(1, 5) if count % n == 0)
    return pl.pallas_call(
        functools.partial(zero_kernel, dims),
        out_shape=jax.ShapeDtypeStruct((dims.groups, dims.slots, dims.bs, dims.bs), jnp.bfloat16),
        out_specs=ANY,
        scratch_shapes=[
            pltpu.VMEM((per, dims.bs, dims.bs), jnp.bfloat16),
            pltpu.SemaphoreType.DMA((dims.groups * count // per,)),
        ],
        compiler_params=pltpu.CompilerParams(vmem_limit_bytes=GRANT),
        name="zero",
    )()


def call_step(dims, left, tile, panels, acc, ahead=None, tiles=()):
    layout, arrays = flat(panels)
    args = [*left, tile, *arrays, *(array for _, array, _ in tiles)]
    aliases = {}
    if acc is not None:
        aliases = {len(args): 0}
        args.append(acc)
    shapes = [jax.ShapeDtypeStruct((dims.rows, dims.bins * dims.bs), jnp.float32)]
    out_specs = [VMEM]
    scratch = scratch_of(dims, panels)
    if ahead is not None:
        shapes.append(jax.ShapeDtypeStruct((dims.rows, dims.rows), jnp.bfloat16))
        out_specs.append(VMEM)
    if tiles:
        small = [(dims.groups * dims.bins,), (dims.groups, 1, dims.slots), (1, dims.groups)]
        shapes += [jax.ShapeDtypeStruct(shape, jnp.int32) for shape in small]
        out_specs += [ANY] * 3
        scratch += [
            pltpu.VMEM((dims.groups * dims.cycle, 128), jnp.int32),
            pltpu.SMEM((dims.groups,), jnp.int32),
            *(pltpu.SMEM(shape, jnp.int32) for shape in small),
            pltpu.SemaphoreType.DMA((3,)),
        ]
    marks = tuple((n, at) for n, _, at in tiles)
    return pl.pallas_call(
        functools.partial(step_kernel, dims, layout, acc is not None, ahead, marks),
        out_shape=shapes,
        in_specs=[VMEM] * len(args),
        out_specs=out_specs,
        scratch_shapes=scratch,
        input_output_aliases=aliases,
        compiler_params=pltpu.CompilerParams(vmem_limit_bytes=GRANT),
        cost_estimate=cost_of(dims, panels),
    )(*args)


def call_last(dims, panels, lp, acc, slots, empty):
    layout, arrays = flat(panels)
    args = [*arrays, lp, acc, slots, empty]
    return pl.pallas_call(
        functools.partial(last_kernel, dims, layout),
        out_shape=jax.ShapeDtypeStruct(empty.shape, empty.dtype),
        in_specs=[VMEM] * (len(args) - 2) + [ANY, ANY],
        out_specs=ANY,
        scratch_shapes=scratch_of(dims, panels)[1:]
        + [
            pltpu.VMEM((dims.groups * dims.bins, dims.bs, dims.bs), jnp.bfloat16),
            pltpu.SMEM((dims.groups * dims.bins,), jnp.int32),
            pltpu.SemaphoreType.DMA((dims.groups * dims.bins,)),
            pltpu.SemaphoreType.DMA,
        ],
        input_output_aliases={len(args) - 1: 0},
        compiler_params=pltpu.CompilerParams(vmem_limit_bytes=GRANT),
        cost_estimate=cost_of(dims, panels),
    )(*args)


def xor_move(value, axis, bit):
    return lax.ppermute(value, axis, [(i, i ^ bit) for i in range(lax.axis_size(axis))])


def shifted(value, axis, distance):
    size = lax.axis_size(axis)
    return lax.ppermute(value, axis, [((i - distance) % size, i) for i in range(size)])


def ring_moves(cycle):
    ring = [2 * k for k in range(cycle // 2)] + [2 * k + 1 for k in reversed(range(cycle // 2))]
    up = [(ring[k], ring[(k + 1) % cycle]) for k in range(cycle)]
    return up, [(b, a) for a, b in up]


def one_of(values, wanted):
    return jnp.any(values[..., None] == wanted, axis=-2)


def window_index(dims, tile, window):
    groups, per_group, bins, cycle = dims.groups, dims.per_group, dims.bins, dims.cycle
    p = lax.axis_index("rows").astype(jnp.int32)
    c = lax.axis_index("cols").astype(jnp.int32)
    lanes = jnp.arange(groups, dtype=jnp.int32)

    def numbers_of(array):
        numbers = array[: groups * per_group].astype(jnp.int32)
        return numbers.reshape(groups, per_group)

    held = jnp.stack(
        [numbers_of(tile[j])[jnp.array([m ^ j for m in range(groups)])] for j in range(groups)], axis=1
    )
    lrel = (held - (p - HP)) % cycle
    zero = (p - 2 * HP) % cycle if bins < cycle else jnp.int32(0)
    bin_ids = jnp.arange(bins, dtype=jnp.int32)
    bin_abs = (zero + bin_ids) % cycle
    has = jnp.stack([one_of((numbers_of(w[2 * dims.half]) - zero) % cycle, bin_ids) for w in window])
    uses = one_of(lrel, jnp.arange(2 * HP, dtype=jnp.int32))
    hits = jnp.any(uses.transpose(0, 2, 1)[..., None] & has[None], axis=(1, 2))
    counts = jnp.sum(hits.astype(jnp.int32), axis=-1)
    all_totals = lax.all_gather(jnp.sum(counts).reshape(1), "rows", axis=0, tiled=True)
    earlier = jnp.sum(jnp.where(jnp.arange(cycle, dtype=jnp.int32) < p, all_totals, 0))
    lower = bin_abs[:, None] < bin_abs[None, :]
    rank_in = jnp.sum((hits[:, :, None] & lower[None]).astype(jnp.int32), axis=1)
    rank_out = jnp.sum((~hits[:, :, None] & lower[None]).astype(jnp.int32), axis=1)
    slots = jnp.where(hits, rank_in, counts[:, None] + rank_out)
    at_slot = hits[:, None, :] & (slots[:, None, :] == jnp.arange(dims.slots, dtype=jnp.int32)[:, None])
    columns = jnp.sum(jnp.where(at_slot, bin_abs * groups + c + 1, 0), axis=-1) - 1
    pick = (lanes[:, None] ^ c) == lanes[None, :]
    columns = jnp.sum(jnp.where(pick[:, :, None], columns[None], 0), axis=1)
    before = (lanes[None, :] ^ c) < lanes[:, None]
    starts = earlier + jnp.sum(jnp.where(before, counts[None, :], 0), axis=1)
    return slots.reshape(-1), columns[:, None].astype(jnp.int32), starts[:, None].astype(jnp.int32)


def on_device(blocks, block_cols):
    panel_rows, _, per_group, bs, _ = blocks.shape
    groups = lax.axis_size("cols")
    cycle = lax.axis_size("rows")
    if groups != 4 or panel_rows != groups or cycle > 256 or cycle < 2 * HP:
        raise ValueError("unsupported sizes")
    dims = Dims(groups, per_group, bs, min(cycle, 4 * HP - 1), cycle)

    def payload(rows):
        return jax.ShapeDtypeStruct((rows, bs), jnp.bfloat16)

    params = pltpu.CompilerParams(vmem_limit_bytes=GRANT)
    cols = [block_cols] + [xor_move(block_cols, "cols", j) for j in range(1, groups)]
    cols = [jnp.transpose(x, (2, 1, 0)) for x in cols]
    cols[0] = pltpu.with_memory_space_constraint(cols[0], pltpu.HBM)
    flat_blocks = pltpu.with_memory_space_constraint(blocks.reshape(-1, bs), pltpu.HBM)
    own, bare_a, bare_b = pl.pallas_call(
        functools.partial(prep_kernel, dims),
        out_shape=[payload(2 * dims.half)] + [payload(dims.half)] * 2,
        in_specs=[ANY],
        out_specs=[VMEM] * 3,
        scratch_shapes=[pltpu.SemaphoreType.DMA((groups, 2))],
        compiler_params=params,
        name="prep",
    )(flat_blocks)
    own_a, own_b, tile = pl.pallas_call(
        functools.partial(number_kernel, dims),
        out_shape=[payload(dims.half + IDX)] * 2 + [payload(IDX)],
        in_specs=[ANY] * groups + [VMEM] * 2,
        out_specs=[VMEM] * 3,
        scratch_shapes=[
            pltpu.SMEM((groups, per_group, 1, groups), jnp.int32),
            pltpu.SemaphoreType.DMA((groups,)),
        ],
        compiler_params=params,
        name="numbers",
    )(*cols, bare_a, bare_b)

    if dims.whole:
        up, down = ring_moves(cycle)
        pa, pb, qa, qb = [bare_a], [own_b], [own_a], [bare_b]
        for k in range(1, HP + 1):
            pa.append(lax.ppermute(pa[-1], "rows", up))
            qb.append(lax.ppermute(qb[-1], "rows", down))
            if k < HP:
                pb.append(lax.ppermute(pb[-1], "rows", up))
                qa.append(lax.ppermute(qa[-1], "rows", down))
    else:
        sent = jnp.concatenate([bare_a, own_b], axis=0)
        window = [sent if k == 0 else shifted(sent, "rows", -k) for k in range(-HP, HP)]
    left1 = xor_move(own, "cols", 1)
    left2 = xor_move(own, "cols", 2)
    left3 = xor_move(left2, "cols", 1)
    left = [own, left1, left2, left3]

    if dims.whole:
        far = lax.ppermute(tile, "rows", [(a, dict(up)[dict(up)[dict(up)[b]]]) for a, b in up])
        pairs = [[(-k, pa[k], pb[k], "b"), (k, qa[k], qb[k], "a")] for k in range(1, HP)]
        first = [(0, bare_a, own_b, "b")] + pairs[0]
        acc, lp = call_step(dims, left, tile, first, None, ahead=HP)
        acc = call_step(dims, left, tile, pairs[1], acc)[0]
        tiles = [(0, tile, 0), (HP, far, 0)]
        for k in range(1, HP):
            tiles += [(cycle - k, pb[k], dims.half), (k, qa[k], dims.half)]
        acc, slots, columns, starts = call_step(dims, left, tile, pairs[2], acc, tiles=tiles)
        starts = starts.reshape(groups, 1)
        final = [(HP, pa[HP], qb[HP], far)]
    else:
        slots, columns, starts = window_index(dims, tile, window)
        pairs = [(k, window[k + HP], None, "a") for k in range(-HP, HP)]
        acc, lp = call_step(dims, left, tile, pairs[:1], None, ahead=HP - 1)
        for k in range(1, len(pairs) - 1, 2):
            acc = call_step(dims, left, tile, pairs[k : k + 2], acc)[0]
        final = pairs[-1:]
    empty = call_zero(dims)
    out = call_last(dims, final, lp, acc, slots, empty)
    return out[:, None], columns, starts


def solution(mesh):
    in_specs = (P("rows", "cols", None, None, None), P("rows", "cols", None))
    out_specs = (P("rows", "cols", None, None, None), P("rows", "cols", None), P("rows", "cols"))

    return jax.shard_map(on_device, mesh=mesh, in_specs=in_specs, out_specs=out_specs, check_vma=False)
```

```python
import functools

import jax
import jax.numpy as jnp
from jax import lax
from jax.experimental import pallas as pl
from jax.experimental.pallas import tpu as pltpu
from jax.sharding import PartitionSpec as P


HP = 4
IDX = 16


VMEM = pl.BlockSpec(memory_space=pltpu.VMEM)
SMEM = pl.BlockSpec(memory_space=pltpu.SMEM)
ANY = pl.BlockSpec(memory_space=pl.ANY)
GRANT = 12 * 1024 * 1024


class Dims:
    def __init__(self, groups, per_group, bs, bins, cycle):
        self.groups, self.per_group, self.bs = groups, per_group, bs
        self.bins, self.cycle = bins, cycle
        self.half = groups // 2 * per_group * bs
        self.rows = groups * bs
        self.slots = groups * per_group * per_group
        self.whole = cycle == 2 * HP and bins == cycle

    def at(self, j, s):
        return (j * self.per_group + s) * self.bs


def ring_place(panel, cycle):
    return jnp.where(panel % 2 == 0, panel // 2, cycle - 1 - panel // 2)


def panel_number(dims, distance):
    me = lax.axis_index("rows").astype(jnp.int32)
    if not dims.whole:
        return (me + distance + dims.cycle) % dims.cycle
    place = (ring_place(me, dims.cycle) + distance + dims.cycle) % dims.cycle
    return jnp.where(place < dims.cycle // 2, 2 * place, 2 * (dims.cycle - 1 - place) + 1)


def first_bin(dims):
    me = lax.axis_index("rows").astype(jnp.int32)
    return (me - 2 * HP + 2 * dims.cycle) % dims.cycle


def stretch(tile, rows):
    return jnp.concatenate([tile] * (rows // 16), axis=0)


def prep_kernel(dims, blocks_ref, full_ref, a_ref, b_ref, sems):
    me = lax.axis_index("cols").astype(jnp.int32)
    span = dims.per_group * dims.bs
    copies = []
    for j in range(dims.groups):
        at = j * span
        ref, start = (a_ref, at) if at < dims.half else (b_ref, at - dims.half)
        for k, (out_ref, first) in enumerate(((ref, start), (full_ref, at))):
            copy = pltpu.make_async_copy(
                blocks_ref.at[pl.ds((me ^ j) * span, span)], out_ref.at[first : first + span], sems.at[j, k]
            )
            copy.start()
            copies.append(copy)
    for copy in copies:
        copy.wait()


def number_kernel(dims, *refs):
    refs = list(refs)
    names = take(refs, dims.groups)
    a_ref, b_ref, a_out, b_out, tile_ref, cols_ref, sems = refs
    copies = []
    for j in range(dims.groups):
        copies.append(pltpu.make_async_copy(names[j], cols_ref.at[j], sems.at[j]))
        copies[-1].start()
    half = dims.half
    for ref, out_ref in ((a_ref, a_out), (b_ref, b_out)):
        out_ref[0:half, :] = ref[...]
    me = lax.axis_index("cols").astype(jnp.int32)
    line = lax.broadcasted_iota(jnp.int32, (IDX, 128), 0)
    lane = lax.broadcasted_iota(jnp.int32, (IDX, 128), 1)
    tile = jnp.zeros((IDX, 128), jnp.int32)
    for copy in copies:
        copy.wait()
    for j in range(dims.groups):
        row = jnp.zeros((IDX, 128), jnp.int32)
        for r in range(dims.groups):
            for s in range(dims.per_group):
                row = jnp.where(lane == r * dims.per_group + s, cols_ref[j, s, 0, me ^ j ^ r], row)
        tile = jnp.where(line == j, row, tile)
    numbers = (tile // dims.groups).astype(jnp.float32).astype(jnp.bfloat16)
    tile_ref[...] = numbers
    for ref in (a_out, b_out):
        ref[half : half + IDX, :] = numbers


def left_matrix(dims, distance, left, tile_ref, lp_ref, first):
    per_group, bs = dims.per_group, dims.bs
    numbers = tile_ref[...].astype(jnp.float32)
    hits = jnp.where(numbers == panel_number(dims, distance).astype(jnp.float32), 1.0, 0.0)
    for j in range(dims.groups):
        for m in range(dims.groups):
            total = None
            for t in range(per_group):
                at = dims.at(m ^ j, t)
                lane = (m ^ j) * per_group + t
                hit = jnp.broadcast_to(hits[j : j + 1, lane : lane + 1], (16, 128)).astype(jnp.bfloat16)
                term = left[j][at : at + bs, :] * stretch(hit, bs)
                total = term if total is None else total + term
            lp_ref[m * bs : (m + 1) * bs, first + j * bs : first + (j + 1) * bs] = total


def accumulate(dims, pieces, lp_ref, d_ref, emit):
    groups, per_group, bs, bins = dims.groups, dims.per_group, dims.bs, dims.bins
    depth = dims.rows
    rows_of = []
    for *_, ref, at in pieces:
        row = ref[at : at + 16, :].astype(jnp.float32)[0:1, :]
        if dims.bins < dims.cycle:
            row = row - first_bin(dims).astype(jnp.float32)
            row = jnp.where(row < 0, row + float(dims.cycle), row)
        rows_of.append(row)
    for first in range(0, bins, 2):
        chunk = range(first, min(first + 2, bins))
        for n, (_, a_ref, b_ref, _, _) in enumerate(pieces):
            for b in chunk:
                hits = jnp.where(rows_of[n] == float(b), 1.0, 0.0)
                for j in range(groups):
                    total = None
                    for s in range(per_group):
                        ref, start = a_ref, dims.at(j, s)
                        if b_ref is not None and j >= groups // 2:
                            ref, start = b_ref, start - dims.half
                        lane = j * per_group + s
                        hit = jnp.broadcast_to(hits[:, lane : lane + 1], (16, 128)).astype(jnp.bfloat16)
                        term = ref[start : start + bs, :] * stretch(hit, bs)
                        total = term if total is None else total + term
                    d_ref[
                        n * depth + j * bs : n * depth + (j + 1) * bs, b * bs : (b + 1) * bs
                    ] = total
        lo, hi = first * bs, (first + len(chunk)) * bs
        emit(lo, hi, jnp.dot(lp_ref[...], d_ref[:, lo:hi], preferred_element_type=jnp.float32))


def take(refs, count):
    return [refs.pop(0) for _ in range(count)]


def take_pieces(dims, refs, layout):
    pieces = []
    for distance, two, where in layout:
        a_ref = refs.pop(0)
        b_ref = refs.pop(0) if two else None
        if where == "far":
            source, at = refs.pop(0), 0
        else:
            source, at = (b_ref if where == "b" else a_ref), dims.half if two else 2 * dims.half
        pieces.append((distance, a_ref, b_ref, source, at))
    return pieces


def zero_kernel(dims, out_ref, blank_ref, sems):
    per = blank_ref.shape[0]
    blank_ref[...] = jnp.zeros_like(blank_ref)
    copies = []
    for i in range(dims.groups):
        for first in range(dims.bins, dims.slots, per):
            copies.append(
                pltpu.make_async_copy(blank_ref, out_ref.at[i, first : first + per], sems.at[len(copies)])
            )
            copies[-1].start()
    for copy in copies:
        copy.wait()


def step_kernel(dims, layout, with_acc, ahead, tiles, *refs):
    refs = list(refs)
    left = take(refs, dims.groups)
    tile_ref = refs.pop(0)
    pieces = take_pieces(dims, refs, layout)
    tile_refs = take(refs, len(tiles))
    acc_ref = refs.pop(0) if with_acc else None
    out_ref = refs.pop(0)
    ahead_ref = refs.pop(0) if ahead is not None else None
    index_refs = take(refs, 3) if tiles else None
    lp_ref, d_ref = take(refs, 2)
    copies = []
    if tiles:
        wide_ref, count_ref, slot_ref, cols_ref, start_ref, sems = refs
        index_work(dims, tiles, tile_refs, wide_ref, slot_ref, cols_ref, start_ref, count_ref)
        for k, (ref, out) in enumerate(zip((slot_ref, cols_ref, start_ref), index_refs)):
            copies.append(pltpu.make_async_copy(ref, out, sems.at[k]))
            copies[-1].start()

    def emit(lo, hi, value):
        out_ref[:, lo:hi] = value if acc_ref is None else acc_ref[:, lo:hi] + value

    for n, (distance, *_) in enumerate(pieces):
        left_matrix(dims, distance, left, tile_ref, lp_ref, n * dims.rows)
    accumulate(dims, pieces, lp_ref, d_ref, emit)
    if ahead is not None:
        left_matrix(dims, ahead, left, tile_ref, ahead_ref, 0)
    for copy in copies:
        copy.wait()


def last_kernel(dims, layout, *refs):
    refs = list(refs)
    pieces = take_pieces(dims, refs, layout)
    lp_ref, acc_ref, slots_ref, _, out_ref, d_ref, stage_ref, slot_ref, sems, sem = refs
    groups, bs, bins = dims.groups, dims.bs, dims.bins
    me = lax.axis_index("cols").astype(jnp.int32)
    slots = pltpu.make_async_copy(slots_ref, slot_ref, sem)
    slots.start()
    copies = []

    def emit(lo, hi, value):
        value = (acc_ref[:, lo:hi] + value).astype(jnp.bfloat16)
        if lo == 0:
            slots.wait()
        for b in range(lo // bs, hi // bs):
            for m in range(groups):
                k = m * bins + b
                at = b * bs - lo
                stage_ref[k] = value[m * bs : (m + 1) * bs, at : at + bs]
                copy = pltpu.make_async_copy(
                    stage_ref.at[k], out_ref.at[m ^ me, slot_ref[k]], sems.at[k]
                )
                copy.start()
                copies.append(copy)

    accumulate(dims, pieces, lp_ref, d_ref, emit)
    for copy in copies:
        copy.wait()


def index_work(dims, tiles, tile_refs, wide_ref, slot_ref, cols_ref, start_ref, count_ref):
    groups, per_group, bins, cycle = dims.groups, dims.per_group, dims.bins, dims.cycle
    p = lax.axis_index("rows").astype(jnp.int32)
    c = lax.axis_index("cols").astype(jnp.int32)
    for (n, at), ref in zip(tiles, tile_refs):
        tile = ref[at : at + IDX, :].astype(jnp.float32).astype(jnp.int32)
        for j in range(groups):
            wide_ref[j * cycle + n : j * cycle + n + 1, :] = tile[j : j + 1]
    held = [wide_ref[j * cycle : (j + 1) * cycle, :] for j in range(groups)]
    bit = jnp.int32(1) << held[0]
    found = []
    for j in range(groups):
        lanes = range(j * per_group, (j + 1) * per_group)
        union = functools.reduce(jnp.bitwise_or, [bit[:, k : k + 1] for k in lanes])
        union = jnp.broadcast_to(union, (cycle, 128))
        look = jnp.zeros((cycle, 128), jnp.int32)
        for n in range(cycle):
            row = jnp.broadcast_to(union[n : n + 1, :], (cycle, 128))
            look = jnp.where(held[j] == panel_number(dims, n), row, look)
        found.append(look)
    panels = panel_number(dims, lax.broadcasted_iota(jnp.int32, (cycle, 1), 0))
    total = jnp.zeros((cycle, 1), jnp.int32)
    for m in range(groups):
        picks = []
        for j in range(groups):
            for t in range(per_group):
                lane = (m ^ j) * per_group + t
                picks.append(found[j][:, lane : lane + 1])
        bits = functools.reduce(jnp.bitwise_or, picks)
        for b in range(bins):
            total = total + ((bits >> b) & 1)
        mine = bits[0, 0]
        count = jnp.int32(0)
        for b in range(bins):
            count = count + ((mine >> b) & 1)
        count_ref[m ^ c] = count
        used = jnp.int32(0)
        for b in range(bins):
            one = (mine >> b) & 1
            slot = jnp.where(one == 1, used, count + b - used)
            slot_ref[m * bins + b] = slot
            cols_ref[m ^ c, 0, slot] = jnp.where(one == 1, b * groups + c, -1)
            used = used + one
    earlier = jnp.sum(jnp.where(panels < p, total, 0))
    for i in range(groups):
        start_ref[0, i] = earlier
        earlier = earlier + count_ref[i]
        for o in range(bins, dims.slots):
            cols_ref[i, 0, o] = -1


def flat(panels):
    layout, arrays = [], []
    for distance, first, second, where in panels:
        two = second is not None
        layout.append((distance, two, where if isinstance(where, str) else "far"))
        arrays += [first] + [second] * two + [where] * (not isinstance(where, str))
    return layout, arrays


def scratch_of(dims, panels):
    depth = dims.rows * len(panels)
    return [
        pltpu.VMEM((dims.rows, depth), jnp.bfloat16),
        pltpu.VMEM((depth, dims.bins * dims.bs), jnp.bfloat16),
    ]


def cost_of(dims, panels):
    flops = 2 * dims.rows * dims.rows * len(panels) * dims.bins * dims.bs
    return pl.CostEstimate(flops=flops, bytes_accessed=4_000_000, transcendentals=0)


def call_zero(dims):
    count = dims.slots - dims.bins
    per = max(n for n in range(1, 5) if count % n == 0)
    return pl.pallas_call(
        functools.partial(zero_kernel, dims),
        out_shape=jax.ShapeDtypeStruct((dims.groups, dims.slots, dims.bs, dims.bs), jnp.bfloat16),
        out_specs=ANY,
        scratch_shapes=[
            pltpu.VMEM((per, dims.bs, dims.bs), jnp.bfloat16),
            pltpu.SemaphoreType.DMA((dims.groups * count // per,)),
        ],
        compiler_params=pltpu.CompilerParams(vmem_limit_bytes=GRANT),
        name="zero",
    )()


def call_step(dims, left, tile, panels, acc, ahead=None, tiles=()):
    layout, arrays = flat(panels)
    args = [*left, tile, *arrays, *(array for _, array, _ in tiles)]
    aliases = {}
    if acc is not None:
        aliases = {len(args): 0}
        args.append(acc)
    shapes = [jax.ShapeDtypeStruct((dims.rows, dims.bins * dims.bs), jnp.float32)]
    out_specs = [VMEM]
    scratch = scratch_of(dims, panels)
    if ahead is not None:
        shapes.append(jax.ShapeDtypeStruct((dims.rows, dims.rows), jnp.bfloat16))
        out_specs.append(VMEM)
    if tiles:
        small = [(dims.groups * dims.bins,), (dims.groups, 1, dims.slots), (1, dims.groups)]
        shapes += [jax.ShapeDtypeStruct(shape, jnp.int32) for shape in small]
        out_specs += [ANY] * 3
        scratch += [
            pltpu.VMEM((dims.groups * dims.cycle, 128), jnp.int32),
            pltpu.SMEM((dims.groups,), jnp.int32),
            *(pltpu.SMEM(shape, jnp.int32) for shape in small),
            pltpu.SemaphoreType.DMA((3,)),
        ]
    marks = tuple((n, at) for n, _, at in tiles)
    return pl.pallas_call(
        functools.partial(step_kernel, dims, layout, acc is not None, ahead, marks),
        out_shape=shapes,
        in_specs=[VMEM] * len(args),
        out_specs=out_specs,
        scratch_shapes=scratch,
        input_output_aliases=aliases,
        compiler_params=pltpu.CompilerParams(vmem_limit_bytes=GRANT),
        cost_estimate=cost_of(dims, panels),
    )(*args)


def call_last(dims, panels, lp, acc, slots, empty):
    layout, arrays = flat(panels)
    args = [*arrays, lp, acc, slots, empty]
    return pl.pallas_call(
        functools.partial(last_kernel, dims, layout),
        out_shape=jax.ShapeDtypeStruct(empty.shape, empty.dtype),
        in_specs=[VMEM] * (len(args) - 2) + [ANY, ANY],
        out_specs=ANY,
        scratch_shapes=scratch_of(dims, panels)[1:]
        + [
            pltpu.VMEM((dims.groups * dims.bins, dims.bs, dims.bs), jnp.bfloat16),
            pltpu.SMEM((dims.groups * dims.bins,), jnp.int32),
            pltpu.SemaphoreType.DMA((dims.groups * dims.bins,)),
            pltpu.SemaphoreType.DMA,
        ],
        input_output_aliases={len(args) - 1: 0},
        compiler_params=pltpu.CompilerParams(vmem_limit_bytes=GRANT),
        cost_estimate=cost_of(dims, panels),
    )(*args)


def xor_move(value, axis, bit):
    return lax.ppermute(value, axis, [(i, i ^ bit) for i in range(lax.axis_size(axis))])


def shifted(value, axis, distance):
    size = lax.axis_size(axis)
    return lax.ppermute(value, axis, [((i - distance) % size, i) for i in range(size)])


def ring_moves(cycle):
    ring = [2 * k for k in range(cycle // 2)] + [2 * k + 1 for k in reversed(range(cycle // 2))]
    up = [(ring[k], ring[(k + 1) % cycle]) for k in range(cycle)]
    return up, [(b, a) for a, b in up]


def one_of(values, wanted):
    return jnp.any(values[..., None] == wanted, axis=-2)


def window_index(dims, tile, window):
    groups, per_group, bins, cycle = dims.groups, dims.per_group, dims.bins, dims.cycle
    p = lax.axis_index("rows").astype(jnp.int32)
    c = lax.axis_index("cols").astype(jnp.int32)
    lanes = jnp.arange(groups, dtype=jnp.int32)

    def numbers_of(array):
        numbers = array[: groups * per_group].astype(jnp.int32)
        return numbers.reshape(groups, per_group)

    held = jnp.stack(
        [numbers_of(tile[j])[jnp.array([m ^ j for m in range(groups)])] for j in range(groups)], axis=1
    )
    lrel = (held - (p - HP)) % cycle
    zero = (p - 2 * HP) % cycle if bins < cycle else jnp.int32(0)
    bin_ids = jnp.arange(bins, dtype=jnp.int32)
    bin_abs = (zero + bin_ids) % cycle
    has = jnp.stack([one_of((numbers_of(w[2 * dims.half]) - zero) % cycle, bin_ids) for w in window])
    uses = one_of(lrel, jnp.arange(2 * HP, dtype=jnp.int32))
    hits = jnp.any(uses.transpose(0, 2, 1)[..., None] & has[None], axis=(1, 2))
    counts = jnp.sum(hits.astype(jnp.int32), axis=-1)
    all_totals = lax.all_gather(jnp.sum(counts).reshape(1), "rows", axis=0, tiled=True)
    earlier = jnp.sum(jnp.where(jnp.arange(cycle, dtype=jnp.int32) < p, all_totals, 0))
    lower = bin_abs[:, None] < bin_abs[None, :]
    rank_in = jnp.sum((hits[:, :, None] & lower[None]).astype(jnp.int32), axis=1)
    rank_out = jnp.sum((~hits[:, :, None] & lower[None]).astype(jnp.int32), axis=1)
    slots = jnp.where(hits, rank_in, counts[:, None] + rank_out)
    at_slot = hits[:, None, :] & (slots[:, None, :] == jnp.arange(dims.slots, dtype=jnp.int32)[:, None])
    columns = jnp.sum(jnp.where(at_slot, bin_abs * groups + c + 1, 0), axis=-1) - 1
    pick = (lanes[:, None] ^ c) == lanes[None, :]
    columns = jnp.sum(jnp.where(pick[:, :, None], columns[None], 0), axis=1)
    before = (lanes[None, :] ^ c) < lanes[:, None]
    starts = earlier + jnp.sum(jnp.where(before, counts[None, :], 0), axis=1)
    return slots.reshape(-1), columns[:, None].astype(jnp.int32), starts[:, None].astype(jnp.int32)


def on_device(blocks, block_cols):
    panel_rows, _, per_group, bs, _ = blocks.shape
    groups = lax.axis_size("cols")
    cycle = lax.axis_size("rows")
    if groups != 4 or panel_rows != groups or cycle > 256 or cycle < 2 * HP:
        raise ValueError("unsupported sizes")
    dims = Dims(groups, per_group, bs, min(cycle, 4 * HP - 1), cycle)

    def payload(rows):
        return jax.ShapeDtypeStruct((rows, bs), jnp.bfloat16)

    params = pltpu.CompilerParams(vmem_limit_bytes=GRANT)
    cols = [block_cols] + [xor_move(block_cols, "cols", j) for j in range(1, groups)]
    cols = [jnp.transpose(x, (2, 1, 0)) for x in cols]
    cols[0] = pltpu.with_memory_space_constraint(cols[0], pltpu.HBM)
    flat_blocks = pltpu.with_memory_space_constraint(blocks.reshape(-1, bs), pltpu.HBM)
    own, bare_a, bare_b = pl.pallas_call(
        functools.partial(prep_kernel, dims),
        out_shape=[payload(2 * dims.half)] + [payload(dims.half)] * 2,
        in_specs=[ANY],
        out_specs=[VMEM] * 3,
        scratch_shapes=[pltpu.SemaphoreType.DMA((groups, 2))],
        compiler_params=params,
        name="prep",
    )(flat_blocks)
    own_a, own_b, tile = pl.pallas_call(
        functools.partial(number_kernel, dims),
        out_shape=[payload(dims.half + IDX)] * 2 + [payload(IDX)],
        in_specs=[ANY] * groups + [VMEM] * 2,
        out_specs=[VMEM] * 3,
        scratch_shapes=[
            pltpu.SMEM((groups, per_group, 1, groups), jnp.int32),
            pltpu.SemaphoreType.DMA((groups,)),
        ],
        compiler_params=params,
        name="numbers",
    )(*cols, bare_a, bare_b)

    if dims.whole:
        up, down = ring_moves(cycle)
        pa, pb, qa, qb = [bare_a], [own_b], [own_a], [bare_b]
        for k in range(1, HP + 1):
            pa.append(lax.ppermute(pa[-1], "rows", up))
            qb.append(lax.ppermute(qb[-1], "rows", down))
            if k < HP:
                pb.append(lax.ppermute(pb[-1], "rows", up))
                qa.append(lax.ppermute(qa[-1], "rows", down))
    else:
        sent = jnp.concatenate([bare_a, own_b], axis=0)
        window = [sent if k == 0 else shifted(sent, "rows", -k) for k in range(-HP, HP)]
    left1 = xor_move(own, "cols", 1)
    left2 = xor_move(own, "cols", 2)
    left3 = xor_move(left2, "cols", 1)
    left = [own, left1, left2, left3]

    if dims.whole:
        far = lax.ppermute(tile, "rows", [(a, dict(up)[dict(up)[dict(up)[b]]]) for a, b in up])
        pairs = [[(-k, pa[k], pb[k], "b"), (k, qa[k], qb[k], "a")] for k in range(1, HP)]
        acc, lp = call_step(dims, left, tile, [(0, bare_a, own_b, "b")], None, ahead=HP)
        acc = call_step(dims, left, tile, pairs[0] + pairs[1], acc)[0]
        tiles = [(0, tile, 0), (HP, far, 0)]
        for k in range(1, HP):
            tiles += [(cycle - k, pb[k], dims.half), (k, qa[k], dims.half)]
        acc, slots, columns, starts = call_step(dims, left, tile, pairs[2], acc, tiles=tiles)
        starts = starts.reshape(groups, 1)
        final = [(HP, pa[HP], qb[HP], far)]
    else:
        slots, columns, starts = window_index(dims, tile, window)
        pairs = [(k, window[k + HP], None, "a") for k in range(-HP, HP)]
        acc, lp = call_step(dims, left, tile, pairs[:1], None, ahead=HP - 1)
        for k in range(1, len(pairs) - 1, 2):
            acc = call_step(dims, left, tile, pairs[k : k + 2], acc)[0]
        final = pairs[-1:]
    empty = call_zero(dims)
    out = call_last(dims, final, lp, acc, slots, empty)
    return out[:, None], columns, starts


def solution(mesh):
    in_specs = (P("rows", "cols", None, None, None), P("rows", "cols", None))
    out_specs = (P("rows", "cols", None, None, None), P("rows", "cols", None), P("rows", "cols"))

    return jax.shard_map(on_device, mesh=mesh, in_specs=in_specs, out_specs=out_specs, check_vma=False)
```

```python
import functools

import jax
import jax.numpy as jnp
from jax import lax
from jax.experimental import pallas as pl
from jax.experimental.pallas import tpu as pltpu
from jax.sharding import PartitionSpec as P


HP = 4
IDX = 16


VMEM = pl.BlockSpec(memory_space=pltpu.VMEM)
SMEM = pl.BlockSpec(memory_space=pltpu.SMEM)
ANY = pl.BlockSpec(memory_space=pl.ANY)
GRANT = 12 * 1024 * 1024


class Dims:
    def __init__(self, groups, per_group, bs, bins, cycle):
        self.groups, self.per_group, self.bs = groups, per_group, bs
        self.bins, self.cycle = bins, cycle
        self.half = groups // 2 * per_group * bs
        self.rows = groups * bs
        self.slots = groups * per_group * per_group
        self.whole = cycle == 2 * HP and bins == cycle

    def at(self, j, s):
        return (j * self.per_group + s) * self.bs


def ring_place(panel, cycle):
    return jnp.where(panel % 2 == 0, panel // 2, cycle - 1 - panel // 2)


def panel_number(dims, distance):
    me = lax.axis_index("rows").astype(jnp.int32)
    if not dims.whole:
        return (me + distance + dims.cycle) % dims.cycle
    place = (ring_place(me, dims.cycle) + distance + dims.cycle) % dims.cycle
    return jnp.where(place < dims.cycle // 2, 2 * place, 2 * (dims.cycle - 1 - place) + 1)


def first_bin(dims):
    me = lax.axis_index("rows").astype(jnp.int32)
    return (me - 2 * HP + 2 * dims.cycle) % dims.cycle


def stretch(tile, rows):
    return jnp.concatenate([tile] * (rows // 16), axis=0)


def prep_kernel(dims, blocks_ref, a_ref, b_ref, sems):
    me = lax.axis_index("cols").astype(jnp.int32)
    span = dims.per_group * dims.bs
    copies = []
    for j in range(dims.groups):
        at = j * span
        ref, start = (a_ref, at) if at < dims.half else (b_ref, at - dims.half)
        copy = pltpu.make_async_copy(
            blocks_ref.at[pl.ds((me ^ j) * span, span)], ref.at[start : start + span], sems.at[j]
        )
        copy.start()
        copies.append(copy)
    for copy in copies:
        copy.wait()


def number_kernel(dims, *refs):
    refs = list(refs)
    names = take(refs, dims.groups)
    a_ref, b_ref, full_ref, a_out, b_out, tile_ref, cols_ref, sems = refs
    copies = []
    for j in range(dims.groups):
        copies.append(pltpu.make_async_copy(names[j], cols_ref.at[j], sems.at[j]))
        copies[-1].start()
    half = dims.half
    for ref, out_ref, at in ((a_ref, a_out, 0), (b_ref, b_out, half)):
        value = ref[...]
        out_ref[0:half, :] = value
        full_ref[at : at + half, :] = value
    me = lax.axis_index("cols").astype(jnp.int32)
    line = lax.broadcasted_iota(jnp.int32, (IDX, 128), 0)
    lane = lax.broadcasted_iota(jnp.int32, (IDX, 128), 1)
    tile = jnp.zeros((IDX, 128), jnp.int32)
    for copy in copies:
        copy.wait()
    for j in range(dims.groups):
        row = jnp.zeros((IDX, 128), jnp.int32)
        for r in range(dims.groups):
            for s in range(dims.per_group):
                row = jnp.where(lane == r * dims.per_group + s, cols_ref[j, s, 0, me ^ j ^ r], row)
        tile = jnp.where(line == j, row, tile)
    numbers = (tile // dims.groups).astype(jnp.float32).astype(jnp.bfloat16)
    tile_ref[...] = numbers
    for ref in (a_out, b_out):
        ref[half : half + IDX, :] = numbers


def left_matrix(dims, distance, left, tile_ref, lp_ref, first):
    per_group, bs = dims.per_group, dims.bs
    numbers = tile_ref[...].astype(jnp.float32)
    hits = jnp.where(numbers == panel_number(dims, distance).astype(jnp.float32), 1.0, 0.0)
    for j in range(dims.groups):
        for m in range(dims.groups):
            total = None
            for t in range(per_group):
                at = dims.at(m ^ j, t)
                lane = (m ^ j) * per_group + t
                hit = jnp.broadcast_to(hits[j : j + 1, lane : lane + 1], (16, 128)).astype(jnp.bfloat16)
                term = left[j][at : at + bs, :] * stretch(hit, bs)
                total = term if total is None else total + term
            lp_ref[m * bs : (m + 1) * bs, first + j * bs : first + (j + 1) * bs] = total


def accumulate(dims, pieces, lp_ref, d_ref, emit):
    groups, per_group, bs, bins = dims.groups, dims.per_group, dims.bs, dims.bins
    depth = dims.rows
    rows_of = []
    for *_, ref, at in pieces:
        row = ref[at : at + 16, :].astype(jnp.float32)[0:1, :]
        if dims.bins < dims.cycle:
            row = row - first_bin(dims).astype(jnp.float32)
            row = jnp.where(row < 0, row + float(dims.cycle), row)
        rows_of.append(row)
    for first in range(0, bins, 2):
        chunk = range(first, min(first + 2, bins))
        for n, (_, a_ref, b_ref, _, _) in enumerate(pieces):
            for b in chunk:
                hits = jnp.where(rows_of[n] == float(b), 1.0, 0.0)
                for j in range(groups):
                    total = None
                    for s in range(per_group):
                        ref, start = a_ref, dims.at(j, s)
                        if b_ref is not None and j >= groups // 2:
                            ref, start = b_ref, start - dims.half
                        lane = j * per_group + s
                        hit = jnp.broadcast_to(hits[:, lane : lane + 1], (16, 128)).astype(jnp.bfloat16)
                        term = ref[start : start + bs, :] * stretch(hit, bs)
                        total = term if total is None else total + term
                    d_ref[
                        n * depth + j * bs : n * depth + (j + 1) * bs, b * bs : (b + 1) * bs
                    ] = total
        lo, hi = first * bs, (first + len(chunk)) * bs
        emit(lo, hi, jnp.dot(lp_ref[...], d_ref[:, lo:hi], preferred_element_type=jnp.float32))


def take(refs, count):
    return [refs.pop(0) for _ in range(count)]


def take_pieces(dims, refs, layout):
    pieces = []
    for distance, two, where in layout:
        a_ref = refs.pop(0)
        b_ref = refs.pop(0) if two else None
        if where == "far":
            source, at = refs.pop(0), 0
        else:
            source, at = (b_ref if where == "b" else a_ref), dims.half if two else 2 * dims.half
        pieces.append((distance, a_ref, b_ref, source, at))
    return pieces


def zero_kernel(dims, out_ref, blank_ref, sems):
    per = blank_ref.shape[0]
    blank_ref[...] = jnp.zeros_like(blank_ref)
    copies = []
    for i in range(dims.groups):
        for first in range(dims.bins, dims.slots, per):
            copies.append(
                pltpu.make_async_copy(blank_ref, out_ref.at[i, first : first + per], sems.at[len(copies)])
            )
            copies[-1].start()
    for copy in copies:
        copy.wait()


def step_kernel(dims, layout, with_acc, ahead, tiles, *refs):
    refs = list(refs)
    left = take(refs, dims.groups)
    tile_ref = refs.pop(0)
    pieces = take_pieces(dims, refs, layout)
    tile_refs = take(refs, len(tiles))
    acc_ref = refs.pop(0) if with_acc else None
    out_ref = refs.pop(0)
    ahead_ref = refs.pop(0) if ahead is not None else None
    index_refs = take(refs, 3) if tiles else None
    lp_ref, d_ref = take(refs, 2)
    copies = []
    if tiles:
        wide_ref, count_ref, slot_ref, cols_ref, start_ref, sems = refs
        index_work(dims, tiles, tile_refs, wide_ref, slot_ref, cols_ref, start_ref, count_ref)
        for k, (ref, out) in enumerate(zip((slot_ref, cols_ref, start_ref), index_refs)):
            copies.append(pltpu.make_async_copy(ref, out, sems.at[k]))
            copies[-1].start()

    def emit(lo, hi, value):
        out_ref[:, lo:hi] = value if acc_ref is None else acc_ref[:, lo:hi] + value

    for n, (distance, *_) in enumerate(pieces):
        left_matrix(dims, distance, left, tile_ref, lp_ref, n * dims.rows)
    accumulate(dims, pieces, lp_ref, d_ref, emit)
    if ahead is not None:
        left_matrix(dims, ahead, left, tile_ref, ahead_ref, 0)
    for copy in copies:
        copy.wait()


def last_kernel(dims, layout, *refs):
    refs = list(refs)
    pieces = take_pieces(dims, refs, layout)
    lp_ref, acc_ref, slots_ref, _, out_ref, d_ref, stage_ref, slot_ref, sems, sem = refs
    groups, bs, bins = dims.groups, dims.bs, dims.bins
    me = lax.axis_index("cols").astype(jnp.int32)
    slots = pltpu.make_async_copy(slots_ref, slot_ref, sem)
    slots.start()
    copies = []

    def emit(lo, hi, value):
        value = (acc_ref[:, lo:hi] + value).astype(jnp.bfloat16)
        if lo == 0:
            slots.wait()
        for b in range(lo // bs, hi // bs):
            for m in range(groups):
                k = m * bins + b
                at = b * bs - lo
                stage_ref[k] = value[m * bs : (m + 1) * bs, at : at + bs]
                copy = pltpu.make_async_copy(
                    stage_ref.at[k], out_ref.at[m ^ me, slot_ref[k]], sems.at[k]
                )
                copy.start()
                copies.append(copy)

    accumulate(dims, pieces, lp_ref, d_ref, emit)
    for copy in copies:
        copy.wait()


def index_work(dims, tiles, tile_refs, wide_ref, slot_ref, cols_ref, start_ref, count_ref):
    groups, per_group, bins, cycle = dims.groups, dims.per_group, dims.bins, dims.cycle
    p = lax.axis_index("rows").astype(jnp.int32)
    c = lax.axis_index("cols").astype(jnp.int32)
    for (n, at), ref in zip(tiles, tile_refs):
        tile = ref[at : at + IDX, :].astype(jnp.float32).astype(jnp.int32)
        for j in range(groups):
            wide_ref[j * cycle + n : j * cycle + n + 1, :] = tile[j : j + 1]
    held = [wide_ref[j * cycle : (j + 1) * cycle, :] for j in range(groups)]
    bit = jnp.int32(1) << held[0]
    found = []
    for j in range(groups):
        lanes = range(j * per_group, (j + 1) * per_group)
        union = functools.reduce(jnp.bitwise_or, [bit[:, k : k + 1] for k in lanes])
        union = jnp.broadcast_to(union, (cycle, 128))
        look = jnp.zeros((cycle, 128), jnp.int32)
        for n in range(cycle):
            row = jnp.broadcast_to(union[n : n + 1, :], (cycle, 128))
            look = jnp.where(held[j] == panel_number(dims, n), row, look)
        found.append(look)
    panels = panel_number(dims, lax.broadcasted_iota(jnp.int32, (cycle, 1), 0))
    total = jnp.zeros((cycle, 1), jnp.int32)
    for m in range(groups):
        picks = []
        for j in range(groups):
            for t in range(per_group):
                lane = (m ^ j) * per_group + t
                picks.append(found[j][:, lane : lane + 1])
        bits = functools.reduce(jnp.bitwise_or, picks)
        for b in range(bins):
            total = total + ((bits >> b) & 1)
        mine = bits[0, 0]
        count = jnp.int32(0)
        for b in range(bins):
            count = count + ((mine >> b) & 1)
        count_ref[m ^ c] = count
        used = jnp.int32(0)
        for b in range(bins):
            one = (mine >> b) & 1
            slot = jnp.where(one == 1, used, count + b - used)
            slot_ref[m * bins + b] = slot
            cols_ref[m ^ c, 0, slot] = jnp.where(one == 1, b * groups + c, -1)
            used = used + one
    earlier = jnp.sum(jnp.where(panels < p, total, 0))
    for i in range(groups):
        start_ref[0, i] = earlier
        earlier = earlier + count_ref[i]
        for o in range(bins, dims.slots):
            cols_ref[i, 0, o] = -1


def flat(panels):
    layout, arrays = [], []
    for distance, first, second, where in panels:
        two = second is not None
        layout.append((distance, two, where if isinstance(where, str) else "far"))
        arrays += [first] + [second] * two + [where] * (not isinstance(where, str))
    return layout, arrays


def scratch_of(dims, panels):
    depth = dims.rows * len(panels)
    return [
        pltpu.VMEM((dims.rows, depth), jnp.bfloat16),
        pltpu.VMEM((depth, dims.bins * dims.bs), jnp.bfloat16),
    ]


def cost_of(dims, panels):
    flops = 2 * dims.rows * dims.rows * len(panels) * dims.bins * dims.bs
    return pl.CostEstimate(flops=flops, bytes_accessed=4_000_000, transcendentals=0)


def call_zero(dims):
    count = dims.slots - dims.bins
    per = max(n for n in range(1, 5) if count % n == 0)
    return pl.pallas_call(
        functools.partial(zero_kernel, dims),
        out_shape=jax.ShapeDtypeStruct((dims.groups, dims.slots, dims.bs, dims.bs), jnp.bfloat16),
        out_specs=ANY,
        scratch_shapes=[
            pltpu.VMEM((per, dims.bs, dims.bs), jnp.bfloat16),
            pltpu.SemaphoreType.DMA((dims.groups * count // per,)),
        ],
        compiler_params=pltpu.CompilerParams(vmem_limit_bytes=GRANT),
        name="zero",
    )()


def call_step(dims, left, tile, panels, acc, ahead=None, tiles=()):
    layout, arrays = flat(panels)
    args = [*left, tile, *arrays, *(array for _, array, _ in tiles)]
    aliases = {}
    if acc is not None:
        aliases = {len(args): 0}
        args.append(acc)
    shapes = [jax.ShapeDtypeStruct((dims.rows, dims.bins * dims.bs), jnp.float32)]
    out_specs = [VMEM]
    scratch = scratch_of(dims, panels)
    if ahead is not None:
        shapes.append(jax.ShapeDtypeStruct((dims.rows, dims.rows), jnp.bfloat16))
        out_specs.append(VMEM)
    if tiles:
        small = [(dims.groups * dims.bins,), (dims.groups, 1, dims.slots), (1, dims.groups)]
        shapes += [jax.ShapeDtypeStruct(shape, jnp.int32) for shape in small]
        out_specs += [ANY] * 3
        scratch += [
            pltpu.VMEM((dims.groups * dims.cycle, 128), jnp.int32),
            pltpu.SMEM((dims.groups,), jnp.int32),
            *(pltpu.SMEM(shape, jnp.int32) for shape in small),
            pltpu.SemaphoreType.DMA((3,)),
        ]
    marks = tuple((n, at) for n, _, at in tiles)
    return pl.pallas_call(
        functools.partial(step_kernel, dims, layout, acc is not None, ahead, marks),
        out_shape=shapes,
        in_specs=[VMEM] * len(args),
        out_specs=out_specs,
        scratch_shapes=scratch,
        input_output_aliases=aliases,
        compiler_params=pltpu.CompilerParams(vmem_limit_bytes=GRANT),
        cost_estimate=cost_of(dims, panels),
    )(*args)


def call_last(dims, panels, lp, acc, slots, empty):
    layout, arrays = flat(panels)
    args = [*arrays, lp, acc, slots, empty]
    return pl.pallas_call(
        functools.partial(last_kernel, dims, layout),
        out_shape=jax.ShapeDtypeStruct(empty.shape, empty.dtype),
        in_specs=[VMEM] * (len(args) - 2) + [ANY, ANY],
        out_specs=ANY,
        scratch_shapes=scratch_of(dims, panels)[1:]
        + [
            pltpu.VMEM((dims.groups * dims.bins, dims.bs, dims.bs), jnp.bfloat16),
            pltpu.SMEM((dims.groups * dims.bins,), jnp.int32),
            pltpu.SemaphoreType.DMA((dims.groups * dims.bins,)),
            pltpu.SemaphoreType.DMA,
        ],
        input_output_aliases={len(args) - 1: 0},
        compiler_params=pltpu.CompilerParams(vmem_limit_bytes=GRANT),
        cost_estimate=cost_of(dims, panels),
    )(*args)


def xor_move(value, axis, bit):
    return lax.ppermute(value, axis, [(i, i ^ bit) for i in range(lax.axis_size(axis))])


def shifted(value, axis, distance):
    size = lax.axis_size(axis)
    return lax.ppermute(value, axis, [((i - distance) % size, i) for i in range(size)])


def ring_moves(cycle):
    ring = [2 * k for k in range(cycle // 2)] + [2 * k + 1 for k in reversed(range(cycle // 2))]
    up = [(ring[k], ring[(k + 1) % cycle]) for k in range(cycle)]
    return up, [(b, a) for a, b in up]


def one_of(values, wanted):
    return jnp.any(values[..., None] == wanted, axis=-2)


def window_index(dims, tile, window):
    groups, per_group, bins, cycle = dims.groups, dims.per_group, dims.bins, dims.cycle
    p = lax.axis_index("rows").astype(jnp.int32)
    c = lax.axis_index("cols").astype(jnp.int32)
    lanes = jnp.arange(groups, dtype=jnp.int32)

    def numbers_of(array):
        numbers = array[: groups * per_group].astype(jnp.int32)
        return numbers.reshape(groups, per_group)

    held = jnp.stack(
        [numbers_of(tile[j])[jnp.array([m ^ j for m in range(groups)])] for j in range(groups)], axis=1
    )
    lrel = (held - (p - HP)) % cycle
    zero = (p - 2 * HP) % cycle if bins < cycle else jnp.int32(0)
    bin_ids = jnp.arange(bins, dtype=jnp.int32)
    bin_abs = (zero + bin_ids) % cycle
    has = jnp.stack([one_of((numbers_of(w[2 * dims.half]) - zero) % cycle, bin_ids) for w in window])
    uses = one_of(lrel, jnp.arange(2 * HP, dtype=jnp.int32))
    hits = jnp.any(uses.transpose(0, 2, 1)[..., None] & has[None], axis=(1, 2))
    counts = jnp.sum(hits.astype(jnp.int32), axis=-1)
    all_totals = lax.all_gather(jnp.sum(counts).reshape(1), "rows", axis=0, tiled=True)
    earlier = jnp.sum(jnp.where(jnp.arange(cycle, dtype=jnp.int32) < p, all_totals, 0))
    lower = bin_abs[:, None] < bin_abs[None, :]
    rank_in = jnp.sum((hits[:, :, None] & lower[None]).astype(jnp.int32), axis=1)
    rank_out = jnp.sum((~hits[:, :, None] & lower[None]).astype(jnp.int32), axis=1)
    slots = jnp.where(hits, rank_in, counts[:, None] + rank_out)
    at_slot = hits[:, None, :] & (slots[:, None, :] == jnp.arange(dims.slots, dtype=jnp.int32)[:, None])
    columns = jnp.sum(jnp.where(at_slot, bin_abs * groups + c + 1, 0), axis=-1) - 1
    pick = (lanes[:, None] ^ c) == lanes[None, :]
    columns = jnp.sum(jnp.where(pick[:, :, None], columns[None], 0), axis=1)
    before = (lanes[None, :] ^ c) < lanes[:, None]
    starts = earlier + jnp.sum(jnp.where(before, counts[None, :], 0), axis=1)
    return slots.reshape(-1), columns[:, None].astype(jnp.int32), starts[:, None].astype(jnp.int32)


def on_device(blocks, block_cols):
    panel_rows, _, per_group, bs, _ = blocks.shape
    groups = lax.axis_size("cols")
    cycle = lax.axis_size("rows")
    if groups != 4 or panel_rows != groups or cycle > 256 or cycle < 2 * HP:
        raise ValueError("unsupported sizes")
    dims = Dims(groups, per_group, bs, min(cycle, 4 * HP - 1), cycle)

    def payload(rows):
        return jax.ShapeDtypeStruct((rows, bs), jnp.bfloat16)

    params = pltpu.CompilerParams(vmem_limit_bytes=GRANT)
    cols = [block_cols] + [xor_move(block_cols, "cols", j) for j in range(1, groups)]
    cols = [jnp.transpose(x, (2, 1, 0)) for x in cols]
    cols[0] = pltpu.with_memory_space_constraint(cols[0], pltpu.HBM)
    flat_blocks = pltpu.with_memory_space_constraint(blocks.reshape(-1, bs), pltpu.HBM)
    bare_a, bare_b = pl.pallas_call(
        functools.partial(prep_kernel, dims),
        out_shape=[payload(dims.half)] * 2,
        in_specs=[ANY],
        out_specs=[VMEM] * 2,
        scratch_shapes=[pltpu.SemaphoreType.DMA((groups,))],
        compiler_params=params,
        name="prep",
    )(flat_blocks)
    own, own_a, own_b, tile = pl.pallas_call(
        functools.partial(number_kernel, dims),
        out_shape=[payload(2 * dims.half)] + [payload(dims.half + IDX)] * 2 + [payload(IDX)],
        in_specs=[ANY] * groups + [VMEM] * 2,
        out_specs=[VMEM] * 4,
        scratch_shapes=[
            pltpu.SMEM((groups, per_group, 1, groups), jnp.int32),
            pltpu.SemaphoreType.DMA((groups,)),
        ],
        compiler_params=params,
        name="numbers",
    )(*cols, bare_a, bare_b)

    if dims.whole:
        up, down = ring_moves(cycle)
        pa, pb, qa, qb = [bare_a], [own_b], [own_a], [bare_b]
        for k in range(1, HP + 1):
            pa.append(lax.ppermute(pa[-1], "rows", up))
            qb.append(lax.ppermute(qb[-1], "rows", down))
            if k < HP:
                pb.append(lax.ppermute(pb[-1], "rows", up))
                qa.append(lax.ppermute(qa[-1], "rows", down))
    else:
        sent = jnp.concatenate([bare_a, own_b], axis=0)
        window = [sent if k == 0 else shifted(sent, "rows", -k) for k in range(-HP, HP)]
    left1 = xor_move(own, "cols", 1)
    left2 = xor_move(own, "cols", 2)
    left3 = xor_move(left2, "cols", 1)
    left = [own, left1, left2, left3]

    if dims.whole:
        far = lax.ppermute(tile, "rows", [(a, dict(up)[dict(up)[dict(up)[b]]]) for a, b in up])
        pairs = [[(-k, pa[k], pb[k], "b"), (k, qa[k], qb[k], "a")] for k in range(1, HP)]
        first = [(0, bare_a, own_b, "b")] + pairs[0]
        acc, lp = call_step(dims, left, tile, first, None, ahead=HP)
        acc = call_step(dims, left, tile, pairs[1], acc)[0]
        tiles = [(0, tile, 0), (HP, far, 0)]
        for k in range(1, HP):
            tiles += [(cycle - k, pb[k], dims.half), (k, qa[k], dims.half)]
        acc, slots, columns, starts = call_step(dims, left, tile, pairs[2], acc, tiles=tiles)
        starts = starts.reshape(groups, 1)
        final = [(HP, pa[HP], qb[HP], far)]
    else:
        slots, columns, starts = window_index(dims, tile, window)
        pairs = [(k, window[k + HP], None, "a") for k in range(-HP, HP)]
        acc, lp = call_step(dims, left, tile, pairs[:1], None, ahead=HP - 1)
        for k in range(1, len(pairs) - 1, 2):
            acc = call_step(dims, left, tile, pairs[k : k + 2], acc)[0]
        final = pairs[-1:]
    empty = call_zero(dims)
    out = call_last(dims, final, lp, acc, slots, empty)
    return out[:, None], columns, starts


def solution(mesh):
    in_specs = (P("rows", "cols", None, None, None), P("rows", "cols", None))
    out_specs = (P("rows", "cols", None, None, None), P("rows", "cols", None), P("rows", "cols"))

    return jax.shard_map(on_device, mesh=mesh, in_specs=in_specs, out_specs=out_specs, check_vma=False)
```
